32 devices in a mesh: band: 4 (over x, core), fft: 8 (over z, y).
Axes of the slice: x: 2, y: 2, z: 4, core: 2. Of those that a mesh axis runs over, the one named last changes fastest.
Arguments:
- orbitals: bfloat16 [16, 2, 32768], P('band', None, 'fft'), may hold values from -6 to 6
- sphere_slot: int32 [32768], P('fft'), may hold values from 0 to 24575, as said below
- stick_column: int32 [1024], P('fft'), may hold values from 0 to 36863, as said below
- potential: float32 [192, 192, 192], P('fft'), may hold values from -3 to 3
- subspace: bfloat16 [64, 2, 32768], P('band', None, 'fft'), may hold values from -0.03125 to 0.03125
- previous: bfloat16 [16, 2, 32768], P('band', None, 'fft'), may hold values from -6 to 6
Outputs:
- applied: bfloat16 [16, 2, 32768], P('band', None, 'fft')
- intersection: float32 [2, 64, 16], P(None, 'fft', 'band')
The draws below stay inside these ranges and needn't reach their ends.
Inputs may be any that keep to these rules, and one draw needn't show every extreme that they name: `sphere_slot`: within each aligned block of 4096 entries the values are distinct. `stick_column`: aligned block d of 128 entries holds distinct columns x * 192 + y with d * 24 <= x < (d + 1) * 24.
All inputs are finite; a program needn't handle non-finite values.
Results may differ from the reference program's by a relative error of at most 0.012.
Values may be sent and summed in bfloat16 or wider, within the bound.
A program may use at most 64 MiB of HBM per device.

```python
import jax
import jax.numpy as jnp
from jax import lax

NG = 192
STK = 128
NPW_DEV = 4096
SUBB = 64
BANDS = 16
STICKS = 1024
NPW_TOT = 32768


def draw_sphere_slot(key, part):
    blocks = NPW_TOT // NPW_DEV
    keys = jax.random.split(jax.random.fold_in(key, 11), blocks)

    def one_block(block_key):
        return jax.random.permutation(block_key, NG * STK)[:NPW_DEV].astype(jnp.int32)
    return jax.vmap(one_block)(keys).reshape(-1).astype(jnp.int32)


def draw_stick_column(key, part):
    blocks = STICKS // STK
    slab_cells = NG // blocks * NG
    keys = jax.random.split(jax.random.fold_in(key, 23), blocks)

    def one_block(block_key, owner):
        return jax.random.permutation(block_key, slab_cells)[:STK].astype(jnp.int32) + owner * slab_cells
    owners = jnp.arange(blocks, dtype=jnp.int32)
    return jax.vmap(one_block)(keys, owners).reshape(-1).astype(jnp.int32)


def strengthened(result, rng, source, target, shards_of, factor):
    def block_of(axis_at):
        return (jnp.arange(result.shape[axis_at]) // (result.shape[axis_at] // shards_of)).reshape((-1,) + (1,) * (result.ndim - 1 - axis_at))

    first = jax.random.permutation(rng, shards_of)[block_of(target)]
    other_side = (block_of(target) + shards_of // 2) % shards_of
    return jnp.where((block_of(source) == first) | (block_of(source) == other_side), factor * result, result)


def level_of(stream_key, shape, cuts, low, high):
    factor_of, own = 1.0, jax.random.fold_in(stream_key, 6)
    for position, blocks in cuts:
        steps = jnp.exp(jax.random.uniform(jax.random.fold_in(own, position), (blocks,), jnp.float32, low / len(cuts), high / len(cuts)))
        factor_of = factor_of * jnp.repeat(steps, shape[position] // blocks).reshape([-1 if axis == position else 1 for axis in range(len(shape))])
    return factor_of


def scatter_about(own_key, extent, scale, reach, pieces=(), held_as=jnp.bfloat16):
    array = scale * jax.random.normal(own_key, extent, jnp.float32)
    if pieces:
        array = array * level_of(own_key, extent, pieces, -0.22, 0.18)
    return jnp.clip(array, -reach, reach).astype(held_as)


def bell_draw_with(rng, dims, scale, reach, cuts, heavy, kind=jnp.bfloat16):
    values = scale * jax.random.normal(rng, dims, jnp.float32)
    if cuts:
        values = values * level_of(rng, dims, cuts, -0.22, 0.18)
    return jnp.clip(strengthened(values, jax.random.fold_in(rng, 3), *heavy), -reach, reach).astype(kind)


def setup_inputs(seed: int = 0) -> dict:
    seeds = jax.random.split(jax.random.key(seed), 7)
    return {
        "orbitals": scatter_about(seeds[0], (BANDS, 2, NPW_TOT), 1.0, 6.0, ((0, 4), (2, 8))),
        "sphere_slot": draw_sphere_slot(jax.random.fold_in(seeds[6], 71), 0),
        "stick_column": draw_stick_column(jax.random.fold_in(seeds[6], 71), 0),
        "potential": jnp.clip(jax.random.uniform(seeds[3], (NG, NG, NG), jnp.float32, -3.0, 3.0) * level_of(seeds[3], (NG, NG, NG), ((0, 8),), -0.4, 0.0), -3.0, 3.0),
        "subspace": bell_draw_with(seeds[4], (SUBB, 2, NPW_TOT), (2 * NPW_TOT) ** -0.5, 0.03125, ((0, 4), (2, 8)), (2, 0, 8, 2.0)),
        "previous": scatter_about(seeds[5], (BANDS, 2, NPW_TOT), 1.0, 6.0, ((0, 4), (2, 8))),
    }


def frequency(values, grid_size):
    return jnp.where(values >= grid_size // 2, values - grid_size, values).astype(jnp.float32)


def rounded(values):
    real_part = lax.optimization_barrier(jnp.real(values).astype(jnp.bfloat16)).astype(jnp.float32)
    imag_part = lax.optimization_barrier(jnp.imag(values).astype(jnp.bfloat16)).astype(jnp.float32)
    return lax.complex(real_part, imag_part)


def reference(orbitals, sphere_slot, stick_column, potential, subspace, previous):
    owner = jnp.arange(NPW_TOT, dtype=jnp.int32) // NPW_DEV
    plane_index = (sphere_slot // STK).astype(jnp.int32)
    column = stick_column[(owner * STK + sphere_slot % STK).astype(jnp.int32)]
    cell = (plane_index * (NG * NG) + column).astype(jnp.int32)
    freq_z = frequency(plane_index, NG)
    freq_x = frequency(column // NG, NG)
    freq_y = frequency(column % NG, NG)
    kinetic = (freq_z * freq_z + freq_x * freq_x + freq_y * freq_y) * (2.0 / (NG * NG))

    def one_band(coeffs):
        real_in = coeffs[0].astype(jnp.float32)
        imag_in = coeffs[1].astype(jnp.float32)
        empty = jnp.zeros((NG * NG * NG,), jnp.float32)
        grid = lax.complex(empty.at[cell].set(real_in), empty.at[cell].set(imag_in)).reshape(NG, NG, NG)
        grid = rounded(jnp.fft.ifft(grid, axis=0, norm="forward"))
        grid = rounded(jnp.fft.ifft(grid, axis=2, norm="forward"))
        grid = rounded(jnp.fft.ifft(grid, axis=1, norm="forward") * potential)
        grid = rounded(jnp.fft.fft(grid, axis=1, norm="forward"))
        grid = rounded(jnp.fft.fft(grid, axis=2, norm="forward"))
        grid = jnp.fft.fft(grid, axis=0, norm="forward")
        values = grid.reshape(-1)[cell]
        applied_real = jnp.real(values) + kinetic * real_in
        applied_imag = jnp.imag(values) + kinetic * imag_in
        return jnp.stack([applied_real, applied_imag]).astype(jnp.bfloat16)

    applied = lax.map(one_band, orbitals)
    sub_real = subspace[:, 0]
    sub_imag = subspace[:, 1]
    prev_real = previous[:, 0]
    prev_imag = previous[:, 1]
    over_real = jnp.dot(sub_real, prev_real.T, preferred_element_type=jnp.float32) + jnp.dot(sub_imag, prev_imag.T, preferred_element_type=jnp.float32)
    over_imag = jnp.dot(sub_real, prev_imag.T, preferred_element_type=jnp.float32) - jnp.dot(sub_imag, prev_real.T, preferred_element_type=jnp.float32)
    return applied, jnp.stack([over_real, over_imag])
```

```python
import functools
import math

import jax
import jax.numpy as jnp
import numpy as np
from jax import lax
from jax.experimental import pallas as pl
from jax.experimental.pallas import tpu as pltpu
from jax.sharding import PartitionSpec as P


def dft_table(length, sign_value, factor):
    positions = jnp.arange(length, dtype=jnp.int32)
    phase_step = positions[:, None] * positions[None, :] % length
    angle_value = phase_step.astype(jnp.float32) * (2.0 * math.pi / length)
    cosine = (jnp.cos(angle_value) * factor).astype(jnp.bfloat16)
    sine_part = (jnp.sin(angle_value) * (sign_value * factor)).astype(jnp.bfloat16)
    return (cosine, sine_part)


def apply_dft(real_in, imag_in, table, form):
    cosine, sine_part = table

    def product(operand, table_part):
        return jnp.einsum(form, operand, table_part, preferred_element_type=jnp.float32)

    real_out = product(real_in, cosine) - product(imag_in, sine_part)
    imag_out = product(real_in, sine_part) + product(imag_in, cosine)
    return (real_out, imag_out)


def packed(pair, axis_pos):
    return jnp.stack([pair[0].astype(jnp.bfloat16), pair[1].astype(jnp.bfloat16)], axis=axis_pos)


def frequency(values, grid_size):
    return jnp.where(values >= grid_size // 2, values - grid_size, values).astype(jnp.float32)


def one_hot_rows(indices, count):
    return (indices[None, :] == jnp.arange(count, dtype=jnp.int32)[:, None]).astype(jnp.bfloat16)


def general_device(orbitals, sphere_slot, stick_column, potential, subspace, previous):
    slab_depth = potential.shape[0]
    grid_size = potential.shape[1]
    stick_count = stick_column.shape[0]
    slab_cells = slab_depth * grid_size
    forward = dft_table(grid_size, 1.0, 1.0)
    inverse = dft_table(grid_size, -1.0, 1.0 / grid_size)
    plane_index = sphere_slot // stick_count
    stick_index = sphere_slot % stick_count
    plane_hot = one_hot_rows(plane_index, grid_size)
    stick_hot = one_hot_rows(stick_index, stick_count)
    stick_coords = jnp.stack([stick_column // grid_size, stick_column % grid_size]).astype(
        jnp.bfloat16
    )
    wave_coords = jnp.dot(stick_coords, stick_hot, preferred_element_type=jnp.float32)
    freq_z = frequency(plane_index, grid_size)
    freq_x = frequency(wave_coords[0].astype(jnp.int32), grid_size)
    freq_y = frequency(wave_coords[1].astype(jnp.int32), grid_size)
    kinetic = (freq_z * freq_z + freq_x * freq_x + freq_y * freq_y) * (
        2.0 / (grid_size * grid_size)
    )
    prev_real = previous[:, 0]
    prev_imag = previous[:, 1]
    sub_piece = lax.all_gather(subspace, "band", axis=0, tiled=True)
    sub_real = sub_piece[:, 0]
    sub_imag = sub_piece[:, 1]
    over_real = jnp.einsum(
        "jg,ig->ji", sub_real, prev_real, preferred_element_type=jnp.float32
    ) + jnp.einsum("jg,ig->ji", sub_imag, prev_imag, preferred_element_type=jnp.float32)
    over_imag = jnp.einsum(
        "jg,ig->ji", sub_real, prev_imag, preferred_element_type=jnp.float32
    ) - jnp.einsum("jg,ig->ji", sub_imag, prev_real, preferred_element_type=jnp.float32)
    partial_value = jnp.stack([over_real, over_imag])
    intersection = lax.psum_scatter(partial_value, "fft", scatter_dimension=1, tiled=True)
    stick_buffer = jnp.einsum(
        "bpi,zi,si->bpzs", orbitals, plane_hot, stick_hot, preferred_element_type=jnp.float32
    ).astype(jnp.bfloat16)

    def potential_work(along_y):
        along_x = apply_dft(along_y[0], along_y[1], forward, "zxy,xk->zky")
        weighted = packed((along_x[0] * potential, along_x[1] * potential), 0)
        back_x = packed(apply_dft(weighted[0], weighted[1], inverse, "zxy,xk->zky"), 0)
        return packed(apply_dft(back_x[0], back_x[1], inverse, "zxy,yk->zxk"), 0)

    along_z = packed(apply_dft(stick_buffer[:, 0], stick_buffer[:, 1], forward, "bzs,zk->bks"), 1)
    all_columns = lax.all_gather(stick_column, "fft", axis=0, tiled=True)
    owners = all_columns.shape[0] // stick_count
    block_columns = (all_columns % slab_cells).reshape(owners, stick_count)
    block_hot = (
        block_columns[:, :, None] == jnp.arange(slab_cells, dtype=jnp.int32)[None, None, :]
    ).astype(jnp.bfloat16)

    def stick_work(one_band):
        plane_depth = one_band.shape[1]
        split_band = one_band.reshape(2, plane_depth, owners, stick_count)
        plane_grid = jnp.einsum(
            "pzds,dsc->pzdc", split_band, block_hot, preferred_element_type=jnp.float32
        ).astype(jnp.bfloat16)
        plane_grid = plane_grid.reshape(2, plane_depth, grid_size, grid_size)
        along_y = packed(apply_dft(plane_grid[0], plane_grid[1], forward, "zxy,yk->zxk"), 0)
        back_y = potential_work(along_y)
        back_split = back_y.reshape(2, plane_depth, owners, slab_cells)
        picked = jnp.einsum(
            "pzdc,dsc->pzds", back_split, block_hot, preferred_element_type=jnp.float32
        ).astype(jnp.bfloat16)
        return picked.reshape(2, plane_depth, owners * stick_count)

    finished = lax.map(
        stick_work, lax.all_to_all(along_z, "fft", split_axis=2, concat_axis=3, tiled=True)
    )
    stick_values = lax.all_to_all(finished, "fft", split_axis=3, concat_axis=2, tiled=True)
    picked_sticks = jnp.einsum(
        "bpzs,si->bpzi", stick_values, stick_hot, preferred_element_type=jnp.float32
    ).astype(jnp.bfloat16)
    cosine_cols = jnp.einsum("zk,ki->zi", inverse[0], plane_hot, preferred_element_type=jnp.float32)
    sine_cols = jnp.einsum("zk,ki->zi", inverse[1], plane_hot, preferred_element_type=jnp.float32)
    pick_real = picked_sticks[:, 0].astype(jnp.float32)
    pick_imag = picked_sticks[:, 1].astype(jnp.float32)
    wave_real = jnp.sum(pick_real * cosine_cols[None] - pick_imag * sine_cols[None], axis=1)
    wave_imag = jnp.sum(pick_real * sine_cols[None] + pick_imag * cosine_cols[None], axis=1)
    real_out = wave_real + kinetic * orbitals[:, 0].astype(jnp.float32)
    imag_out = wave_imag + kinetic * orbitals[:, 1].astype(jnp.float32)
    applied = jnp.stack([real_out, imag_out], axis=1).astype(jnp.bfloat16)
    return (applied, intersection)


PLANES = 4
PAIR = 2
LANES = 128
CHUNK = 4 * PLANES
EXTRA = 16


def phases(products, length):
    angle = (products % length).astype(np.float64) * (2.0 * np.pi / length)
    return np.cos(angle), np.sin(angle)


def as_bf16(array):
    return jnp.asarray(array, jnp.bfloat16)


def line_tables(length):
    cosine, sine = phases(np.outer(np.arange(length), np.arange(length)), length)

    def spread(table):
        rest = table[:, LANES:]
        return table[:, :LANES], np.concatenate([rest, rest], axis=1)

    tables = []
    for to_real, to_imag in ((cosine, sine), (-sine, cosine)):
        real_main, real_rest = spread(to_real)
        imag_main, imag_rest = spread(to_imag)
        tables.append(np.concatenate([real_main, imag_main, real_rest, imag_rest], axis=1))
    there = np.stack(tables)
    return as_bf16(there), as_bf16(there.transpose(0, 2, 1))


def half_tables(length):
    half = np.arange(length // 2)
    natural = np.arange(length).reshape(2, length // 16, 8)
    mixed = natural.transpose(1, 0, 2).reshape(-1)
    there, back = [], []
    for parity in (0, 1):
        cosine, sine = phases(np.outer(2 * half + parity, half), length)
        table = np.block([[cosine, -sine], [sine, cosine]])
        there.append(table[:, mixed])
        back.append(table.T)
    return as_bf16(np.stack(there + back))


def column_tables(length, slab):
    cosine, sine = phases(np.outer(np.arange(length), np.arange(length)), length)
    table = np.block([[cosine, -sine], [sine, cosine]])
    order = np.arange(2 * length).reshape(2, length // slab, slab // PLANES, PLANES)
    order = order.transpose(2, 1, 0, 3).reshape(-1)
    there = table[order]
    return as_bf16(there), as_bf16(there.T)


def pick_table(slab):
    lines = PLANES * PAIR
    table = np.zeros((CHUNK, lines * slab))
    for plane in range(PLANES):
        for band in range(PAIR):
            line = plane * PAIR + band
            for part in range(2):
                row = band * 2 * PLANES + part * PLANES + plane
                table[row, line * slab : (line + 1) * slab] = 1.0
    return as_bf16(table)


def whole_kernel(
    wave_ref,
    slot_ref,
    coord_ref,
    extra_ref,
    pot_ref,
    deep_ref,
    rise_ref,
    line_ref,
    turn_ref,
    half_ref,
    pick_ref,
    out_ref,
    extra_back_ref,
    full_ref,
    left_ref,
    right_ref,
    hot_ref,
    spread_ref,
    sent_ref,
    stick_ref,
    coords_ref,
    mask_ref,
    there_ref,
    again_ref,
    mixed_ref,
    heavy_ref,
    after_ref,
    kept_ref,
    stage_ref,
    back_ref,
    pot_sem,
    send_sem,
    recv_sem,
    home_send,
    home_recv,
    side_send,
    side_recv,
):
    slab, size, _ = pot_ref.shape
    owners = size // slab
    half_owners = owners // 2
    half = size // 2
    groups_pair = slab // PLANES
    blocks = wave_ref.shape[1]
    sticks = LANES
    lines = PLANES * PAIR
    pairs = wave_ref.shape[0] // (2 * PAIR)
    groups = pairs * groups_pair
    rest = size - LANES
    scale = 1.0 / (size * size)
    me = lax.axis_index("fft")
    others = [lax.rem(me + shift, owners) for shift in range(1, owners)]
    f32, bf16 = jnp.float32, jnp.bfloat16

    def dot(left, right):
        return jnp.dot(left, right, preferred_element_type=f32)

    def remote(src, dst, send, recv, place):
        return pltpu.make_async_remote_copy(
            src_ref=src,
            dst_ref=dst,
            send_sem=send,
            recv_sem=recv,
            device_id={"fft": others[place]},
            device_id_type=pl.DeviceIdType.MESH,
        )

    def coord_copy(place):
        return remote(
            coord_ref, coords_ref.at[me], side_send.at[0, place], side_recv.at[0, place], place
        )

    def extra_copy(place):
        return remote(
            extra_ref.at[others[place]],
            extra_back_ref.at[me],
            side_send.at[1, place],
            side_recv.at[1, place],
            place,
        )

    def there_copy(group, place):
        return remote(
            sent_ref.at[group, others[place]],
            stick_ref.at[group, me],
            send_sem.at[group, place],
            recv_sem.at[group, place],
            place,
        )

    def home_copy(group, place):
        return remote(
            stage_ref.at[group + 2, others[place]],
            back_ref.at[group, me],
            home_send.at[group, place],
            home_recv.at[group, place],
            place,
        )

    main_copy = pltpu.make_async_copy(pot_ref.at[:, :, :LANES], left_ref, pot_sem.at[0])
    rest_copy = pltpu.make_async_copy(pot_ref, full_ref, pot_sem.at[1])
    main_copy.start()
    rest_copy.start()

    barrier = pltpu.get_barrier_semaphore()
    for other in others:
        pl.semaphore_signal(
            barrier, inc=1, device_id={"fft": other}, device_id_type=pl.DeviceIdType.MESH
        )

    low_lane = lax.broadcasted_iota(jnp.int32, (1, LANES), 1) < rest
    level = lax.broadcasted_iota(jnp.int32, (half, LANES), 0)

    @pl.loop(0, blocks, unroll=4)
    def _(block):
        slot = slot_ref[pl.ds(block, 1), :]
        plane = lax.shift_right_logical(slot, 7)
        cell = jnp.where(plane >= half, sticks, 0) + jnp.bitwise_and(slot, sticks - 1)
        rows = lax.broadcasted_iota(jnp.int32, (2 * sticks, LANES), 0)
        place = pl.ds(pl.multiple_of(block * LANES, LANES), LANES)
        hot_ref[:, place] = jnp.where(cell == rows, 1.0, 0.0).astype(bf16)

    pl.semaphore_wait(barrier, owners - 1)
    for place in range(owners - 1):
        coord_copy(place).start()
    for place in range(owners - 1):
        extra_copy(place).start()
    coords_ref[me] = coord_ref[...]
    extra_back_ref[me] = extra_ref[me]

    def level_mask(block):
        plane = lax.shift_right_logical(slot_ref[pl.ds(block, 1), :], 7)
        return jnp.where(plane >= half, plane - half, plane) == level

    @pl.loop(0, pairs)
    def _(pair):
        @pl.loop(0, blocks, unroll=4)
        def _(block):
            chosen = level_mask(block)
            place = pl.ds(pl.multiple_of(block * LANES, LANES), LANES)
            for part in range(2 * PAIR):
                values = wave_ref[2 * PAIR * pair + part, pl.ds(block, 1), :]
                spread_ref[part * half : (part + 1) * half, place] = jnp.where(
                    chosen, values, 0.0
                ).astype(bf16)

        cells = lax.dot_general(
            spread_ref[...], hot_ref[...], (((1,), (1,)), ((), ())), preferred_element_type=f32
        )
        columns = []
        for band in range(PAIR):
            pieces = []
            for part in range(2):
                start = (2 * band + part) * half
                for side in range(2):
                    pieces.append(cells[start : start + half, side * LANES : (side + 1) * LANES])
            columns.append(jnp.concatenate(pieces, axis=0))
        columns = jnp.concatenate(columns, axis=1).astype(bf16)
        along = dot(deep_ref[...], columns).reshape(groups_pair * owners, 2 * PLANES, PAIR * LANES)
        chunks = jnp.concatenate([along[:, :, :LANES], along[:, :, LANES:]], axis=1)
        first = pair * groups_pair
        sent_ref[pl.ds(first, groups_pair)] = chunks.astype(bf16).reshape(
            groups_pair, owners, CHUNK, LANES
        )

        @pl.loop(0, groups_pair)
        def _(step):
            for place in range(owners - 1):
                there_copy(first + step, place).start()
            stick_ref[first + step, me] = sent_ref[first + step, me]

    main_copy.wait()
    rest_copy.wait()

    @pl.loop(0, slab)
    def _(plane):
        local = full_ref[plane, :, LANES:]
        right_ref[plane] = jnp.concatenate([local, local], axis=1)

    for place in range(owners - 1):
        coord_copy(place).wait()

    @pl.loop(0, owners)
    def _(owner):
        coords = coords_ref[owner]
        local = lax.broadcasted_iota(jnp.int32, (slab, sticks), 0).astype(f32)
        mask_ref[owner] = jnp.where(coords[0:1, :] == local, 1.0, 0.0)
        cells = lax.broadcasted_iota(jnp.int32, (size, sticks), 0).astype(f32)
        hot = jnp.where(coords[1:2, :] == cells, 1.0, 0.0).astype(bf16)
        for part in range(2):
            rows = lax.dot_general(
                hot, line_ref[part], (((0,), (0,)), ((), ())), preferred_element_type=f32
            )
            there_ref[owner, part * sticks : (part + 1) * sticks, :] = rows.astype(bf16)
            turned = dot(turn_ref[part], hot)
            again_ref[owner, :, part * sticks : (part + 1) * sticks] = turned.astype(bf16)

    def spread_lines(group):
        for low in range(half_owners):
            results = []
            for owner in (low, low + half_owners):
                values = stick_ref[group, owner].astype(f32)
                mask = mask_ref[owner]
                parts = []
                for part in range(2):
                    pieces = []
                    for plane in range(PLANES):
                        for band in range(PAIR):
                            row = band * 2 * PLANES + part * PLANES + plane
                            pieces.append(values[row : row + 1, :] * mask)
                    parts.append(jnp.concatenate(pieces, axis=0))
                left = jnp.concatenate(parts, axis=1).astype(bf16)
                results.append(dot(left, there_ref[owner]))
            for plane in range(PLANES):
                unit, side = plane // 2, plane % 2
                start = plane * PAIR * slab

                def pieces_of(result):
                    one = result[start : start + slab]
                    two = result[start + slab : start + 2 * slab]
                    found = []
                    for half_lines in (one, two):
                        found.append((half_lines[:, :LANES], half_lines[:, LANES : 2 * LANES]))
                    both = []
                    for offset in (2 * LANES, 3 * LANES):
                        both.append(
                            jnp.where(
                                low_lane,
                                one[:, offset : offset + LANES],
                                two[:, offset : offset + LANES],
                            )
                        )
                    found.append(tuple(both))
                    return found

                near, far = pieces_of(results[0]), pieces_of(results[1])
                offsets = (2 * side * LANES, (2 * side + 1) * LANES, (4 + side) * LANES)
                for (near_re, near_im), (far_re, far_im), offset in zip(near, far, offsets):
                    for parity in range(2):
                        if parity == 0:
                            real, imag = near_re + far_re, near_im + far_im
                        else:
                            real, imag = near_re - far_re, near_im - far_im
                        tile = jnp.concatenate(
                            [real.reshape(-1, 8, LANES), imag.reshape(-1, 8, LANES)], axis=1
                        )
                        mixed_ref[
                            unit,
                            parity,
                            slice(2 * slab * low, 2 * slab * (low + 1)),
                            offset : offset + LANES,
                        ] = tile.reshape(2 * slab, LANES).astype(bf16)

    def forward_lines(group, unit):
        first = lax.rem(group, groups_pair) * PLANES
        if True:
            for parity in range(2):
                picks = pl.ds(parity, half, 2)

                for tile in range(3):
                    result = dot(
                        half_ref[parity],
                        mixed_ref[unit, parity, :, 2 * LANES * tile : 2 * LANES * (tile + 1)],
                    )
                    if tile < 2:
                        local = left_ref[first + 2 * unit + tile, picks, :]
                        local = jnp.concatenate([local, local], axis=1)
                    else:
                        one = right_ref[first + 2 * unit, picks, :]
                        two = right_ref[first + 2 * unit + 1, picks, :]
                        local = jnp.concatenate([one, two], axis=1)
                    heavy_ref[unit, parity, tile, :half] = (result[:half] * local).astype(bf16)
                    heavy_ref[unit, parity, tile, half:] = (result[half:] * local).astype(bf16)

    def backward_lines(unit):
        if True:
            for tile in range(3):
                even = dot(half_ref[2], heavy_ref[unit, 0, tile])
                odd = dot(half_ref[3], heavy_ref[unit, 1, tile])
                for side, values in enumerate((even + odd, even - odd)):
                    for low in range(half_owners):
                        owner = low + side * half_owners
                        for part in range(2):
                            start = part * half + low * slab
                            found = values[start : start + slab]
                            one, two = found[:, :LANES], found[:, LANES:]
                            if tile < 2:
                                rows = pl.ds(
                                    pl.multiple_of((2 * unit + tile) * 2 * slab, 2 * slab), 2 * slab
                                )
                                after_ref[owner, rows, part * LANES : (part + 1) * LANES] = (
                                    jnp.concatenate([one, two], axis=0).astype(bf16)
                                )
                            else:
                                for place, both in enumerate((one, two)):
                                    plane = 2 * unit + place
                                    rows = pl.ds(
                                        pl.multiple_of(plane * 2 * slab, 2 * slab), 2 * slab
                                    )
                                    after_ref[
                                        owner, rows, (2 + part) * LANES : (3 + part) * LANES
                                    ] = jnp.concatenate(
                                        [
                                            jnp.where(low_lane, both, 0.0),
                                            jnp.where(low_lane, 0.0, both),
                                        ],
                                        axis=0,
                                    ).astype(bf16)

    part_row = lax.broadcasted_iota(jnp.int32, (CHUNK, LANES), 0)
    part_row = jnp.bitwise_and(part_row, PLANES) == 0

    def weighed_lines():
        for owner in range(owners):
            result = dot(after_ref[owner], again_ref[owner])
            mask = mask_ref[owner] * scale
            mask = jnp.concatenate([mask, mask], axis=1)[None]
            kept = (result.reshape(lines, slab, 2 * LANES) * mask).reshape(lines * slab, 2 * LANES)
            kept_ref[owner] = kept.astype(bf16)

    def picked_lines(place):
        for owner in range(owners):
            found = dot(pick_ref[...], kept_ref[owner])
            stage_ref[place, owner] = jnp.where(
                part_row, found[:, :LANES], found[:, LANES:]
            ).astype(bf16)

    def wait_group(group):
        for place in range(owners - 1):
            there_copy(group, place).wait()

    def send_home(group):
        for place in range(owners - 1):
            home_copy(group, place).start()
        back_ref[group, me] = stage_ref[group + 2, me]

    wait_group(0)
    spread_lines(0)

    @pl.loop(0, groups)
    def _(group):
        @pl.when(group < groups - 1)
        def _():
            wait_group(group + 1)

        forward_lines(group, 0)
        forward_lines(group, 1)
        picked_lines(group)
        weighed_lines()
        backward_lines(0)
        backward_lines(1)
        spread_lines(lax.rem(group + 1, groups))

        @pl.when(group > 1)
        def _():
            send_home(group - 2)

    picked_lines(groups)
    weighed_lines()
    send_home(groups - 2)
    picked_lines(groups + 1)
    send_home(groups - 1)

    for place in range(owners - 1):
        extra_copy(place).wait()

    @pl.loop(0, pairs)
    def _(pair):
        first = pair * groups_pair

        @pl.loop(0, groups_pair)
        def _(step):
            for place in range(owners - 1):
                home_copy(first + step, place).wait()

        chunks = back_ref[pl.ds(first, groups_pair)].reshape(groups_pair * owners, CHUNK, LANES)
        chunks = chunks.astype(f32)
        columns = []
        for band in range(PAIR):
            rows = chunks[:, band * 2 * PLANES : (band + 1) * 2 * PLANES]
            columns.append(rows.reshape(2 * size, LANES))
        columns = jnp.concatenate(columns, axis=1).astype(bf16)
        risen = (dot(rise_ref[...], columns) * (1.0 / size)).astype(bf16)
        pieces = []
        for band in range(PAIR):
            for part in range(2):
                both = []
                for side in range(2):
                    start = part * size + side * half
                    both.append(risen[start : start + half, band * LANES : (band + 1) * LANES])
                pieces.append(jnp.concatenate(both, axis=1))
        spread_ref[:, : 2 * LANES] = jnp.concatenate(pieces, axis=0)

        @pl.loop(0, blocks // 2, unroll=2)
        def _(step):
            place = pl.ds(pl.multiple_of(step * 2 * LANES, LANES), 2 * LANES)
            values = dot(spread_ref[:, : 2 * LANES], hot_ref[:, place])
            for side in range(2):
                block = 2 * step + side
                chosen = level_mask(block)
                for part in range(2 * PAIR):
                    mine = values[part * half : (part + 1) * half, side * LANES : (side + 1) * LANES]
                    out_ref[2 * PAIR * pair + part, pl.ds(block, 1), :] = jnp.sum(
                        jnp.where(chosen, mine, 0.0), axis=0, keepdims=True
                    )


def whole_work(waves, slots, coords, extra, potential):
    slab, size, _ = potential.shape
    owners = size // slab
    groups_pair = slab // PLANES
    parts, blocks, _ = waves.shape
    pairs = parts // (2 * PAIR)
    groups = pairs * groups_pair
    half = size // 2
    lines = PLANES * PAIR
    deep, rise = column_tables(size, slab)
    line, turn = line_tables(size)
    halves = half_tables(size)
    pick = pick_table(slab)
    in_vmem = pl.BlockSpec(memory_space=pltpu.VMEM)
    anywhere = pl.BlockSpec(memory_space=pl.ANY)
    bf16, f32 = jnp.bfloat16, jnp.float32
    dma = pltpu.SemaphoreType.DMA
    return pl.pallas_call(
        whole_kernel,
        out_shape=(
            jax.ShapeDtypeStruct(waves.shape, f32),
            jax.ShapeDtypeStruct(extra.shape, bf16),
        ),
        in_specs=[in_vmem] * 4 + [anywhere] + [in_vmem] * 6,
        out_specs=(in_vmem, in_vmem),
        scratch_shapes=[
            pltpu.VMEM((slab, size, size), f32),
            pltpu.VMEM((slab, size, LANES), f32),
            pltpu.VMEM((slab, size, LANES), f32),
            pltpu.VMEM((2 * LANES, blocks * LANES), bf16),
            pltpu.VMEM((2 * PAIR * half, blocks * LANES), bf16),
            pltpu.VMEM((groups, owners, CHUNK, LANES), bf16),
            pltpu.VMEM((groups, owners, CHUNK, LANES), bf16),
            pltpu.VMEM((owners, 8, LANES), f32),
            pltpu.VMEM((owners, slab, LANES), f32),
            pltpu.VMEM((owners, 2 * LANES, 4 * LANES), bf16),
            pltpu.VMEM((owners, 4 * LANES, 2 * LANES), bf16),
            pltpu.VMEM((PLANES // 2, 2, size, 6 * LANES), bf16),
            pltpu.VMEM((PLANES // 2, 2, 3, size, 2 * LANES), bf16),
            pltpu.VMEM((owners, lines * slab, 4 * LANES), bf16),
            pltpu.VMEM((owners, lines * slab, 2 * LANES), bf16),
            pltpu.VMEM((groups + 2, owners, CHUNK, LANES), bf16),
            pltpu.VMEM((groups, owners, CHUNK, LANES), bf16),
            dma((2,)),
            dma((groups, owners - 1)),
            dma((groups, owners - 1)),
            dma((groups, owners - 1)),
            dma((groups, owners - 1)),
            dma((2, owners - 1)),
            dma((2, owners - 1)),
        ],
        compiler_params=pltpu.CompilerParams(
            collective_id=0, has_side_effects=True, vmem_limit_bytes=56 * 1024 * 1024
        ),
        cost_estimate=pl.CostEstimate(
            flops=40 * 10**9, bytes_accessed=8 * 10**6, transcendentals=0
        ),
    )(waves, slots, coords, extra, potential, deep, rise, line, turn, halves, pick)


def gathered_bands(array, mesh_bands):
    here = lax.axis_index("band")
    blocks = [array]
    for shift in range(1, mesh_bands):
        pairs = [((src + shift) % mesh_bands, src) for src in range(mesh_bands)]
        blocks.append(lax.ppermute(array, "band", pairs))
    return blocks, here


def overlaps(subspace, previous, mesh_bands, owners):
    blocks, here = gathered_bands(subspace, mesh_bands)
    prev_real, prev_imag = previous[:, 0], previous[:, 1]
    right = jnp.concatenate(
        [
            jnp.concatenate([prev_real, prev_imag], axis=1),
            jnp.concatenate([prev_imag, -prev_real], axis=1),
        ],
        axis=0,
    )
    partials = []
    for block in blocks:
        partials.append(
            jnp.einsum(
                "jg,ig->ji",
                block.reshape(block.shape[0], -1),
                right,
                preferred_element_type=jnp.float32,
            )
        )
    twice = jnp.concatenate(partials + partials, axis=0)
    count = twice.shape[0] // 2
    start = (count - here * subspace.shape[0]) % count
    ordered = lax.dynamic_slice_in_dim(twice, start, count, axis=0)
    split = ordered.reshape(owners, count // owners, 2, previous.shape[0])
    return split.transpose(0, 2, 1, 3)


def fast_device(mesh_bands, orbitals, sphere_slot, stick_column, potential, subspace, previous):
    slab_depth, grid_size, _ = potential.shape
    stick_count = stick_column.shape[0]
    owners = grid_size // slab_depth
    bands = orbitals.shape[0]
    plane_index = sphere_slot // stick_count
    stick_index = sphere_slot % stick_count
    stick_hot = one_hot_rows(stick_index, stick_count)
    stick_x = stick_column // grid_size
    stick_y = stick_column % grid_size
    stick_coords = jnp.stack([stick_x, stick_y]).astype(jnp.bfloat16)
    wave_coords = jnp.dot(stick_coords, stick_hot, preferred_element_type=jnp.float32)
    freq_z = frequency(plane_index, grid_size)
    freq_x = frequency(wave_coords[0].astype(jnp.int32), grid_size)
    freq_y = frequency(wave_coords[1].astype(jnp.int32), grid_size)
    kinetic = (freq_z * freq_z + freq_x * freq_x + freq_y * freq_y) * (
        2.0 / (grid_size * grid_size)
    )
    local_x = stick_x - lax.axis_index("fft") * slab_depth
    coords = jnp.stack([local_x, stick_y]).astype(jnp.float32)
    coords = jnp.pad(coords, ((0, 8 - 2), (0, 0)))
    split = overlaps(subspace, previous, mesh_bands, owners)
    flat = split.reshape(owners, 1, -1)
    high = lax.reduce_precision(flat, 8, 7)
    low = lax.reduce_precision(flat - high, 8, 7)
    both = jnp.concatenate([high, low], axis=2).astype(jnp.bfloat16)
    width = both.shape[2]
    lanes = -(-width // stick_count) * stick_count
    both = jnp.pad(both, ((0, 0), (0, 0), (0, lanes - width)))
    both = both.reshape(owners, -1, stick_count)
    both = jnp.pad(both, ((0, 0), (0, EXTRA - both.shape[1]), (0, 0)))
    waves = orbitals.astype(jnp.float32).reshape(2 * bands, -1, LANES)
    slots = sphere_slot.reshape(-1, LANES)
    found, returned = whole_work(waves, slots, coords, both, potential)
    sums = returned.reshape(owners, -1)[:, :width].astype(jnp.float32)
    sums = jnp.sum(sums, axis=0)
    intersection = (sums[: width // 2] + sums[width // 2 :]).reshape(split.shape[1:])
    found = found.reshape(orbitals.shape)
    applied = (found + kinetic * orbitals.astype(jnp.float32)).astype(jnp.bfloat16)
    return (applied, intersection)


def per_device(mesh_bands, *arrays):
    orbitals, slots, sticks, potential, _, _ = arrays
    slab, size, _ = potential.shape
    owners = size // slab
    fits = slab % 8 == 0 and owners % 2 == 0 and owners * slab == size
    fits = fits and 2 * size == 3 * LANES and sticks.shape[0] == LANES
    fits = fits and orbitals.shape[0] % PAIR == 0 and slots.shape[0] % (2 * LANES) == 0
    if fits:
        return fast_device(mesh_bands, *arrays)
    return general_device(*arrays)


def solution(mesh):
    return jax.shard_map(
        functools.partial(per_device, mesh.shape["band"]),
        mesh=mesh,
        in_specs=(
            P("band", None, "fft"),
            P("fft"),
            P("fft"),
            P("fft", None, None),
            P("band", None, "fft"),
            P("band", None, "fft"),
        ),
        out_specs=(P("band", None, "fft"), P(None, "fft", "band")),
        check_vma=False,
    )
```

```python
import functools
import math

import jax
import jax.numpy as jnp
import numpy as np
from jax import lax
from jax.experimental import pallas as pl
from jax.experimental.pallas import tpu as pltpu
from jax.sharding import PartitionSpec as P


def dft_table(length, sign_value, factor):
    positions = jnp.arange(length, dtype=jnp.int32)
    phase_step = positions[:, None] * positions[None, :] % length
    angle_value = phase_step.astype(jnp.float32) * (2.0 * math.pi / length)
    cosine = (jnp.cos(angle_value) * factor).astype(jnp.bfloat16)
    sine_part = (jnp.sin(angle_value) * (sign_value * factor)).astype(jnp.bfloat16)
    return (cosine, sine_part)


def apply_dft(real_in, imag_in, table, form):
    cosine, sine_part = table

    def product(operand, table_part):
        return jnp.einsum(form, operand, table_part, preferred_element_type=jnp.float32)

    real_out = product(real_in, cosine) - product(imag_in, sine_part)
    imag_out = product(real_in, sine_part) + product(imag_in, cosine)
    return (real_out, imag_out)


def packed(pair, axis_pos):
    return jnp.stack([pair[0].astype(jnp.bfloat16), pair[1].astype(jnp.bfloat16)], axis=axis_pos)


def frequency(values, grid_size):
    return jnp.where(values >= grid_size // 2, values - grid_size, values).astype(jnp.float32)


def one_hot_rows(indices, count):
    return (indices[None, :] == jnp.arange(count, dtype=jnp.int32)[:, None]).astype(jnp.bfloat16)


def general_device(orbitals, sphere_slot, stick_column, potential, subspace, previous):
    slab_depth = potential.shape[0]
    grid_size = potential.shape[1]
    stick_count = stick_column.shape[0]
    slab_cells = slab_depth * grid_size
    forward = dft_table(grid_size, 1.0, 1.0)
    inverse = dft_table(grid_size, -1.0, 1.0 / grid_size)
    plane_index = sphere_slot // stick_count
    stick_index = sphere_slot % stick_count
    plane_hot = one_hot_rows(plane_index, grid_size)
    stick_hot = one_hot_rows(stick_index, stick_count)
    stick_coords = jnp.stack([stick_column // grid_size, stick_column % grid_size]).astype(
        jnp.bfloat16
    )
    wave_coords = jnp.dot(stick_coords, stick_hot, preferred_element_type=jnp.float32)
    freq_z = frequency(plane_index, grid_size)
    freq_x = frequency(wave_coords[0].astype(jnp.int32), grid_size)
    freq_y = frequency(wave_coords[1].astype(jnp.int32), grid_size)
    kinetic = (freq_z * freq_z + freq_x * freq_x + freq_y * freq_y) * (
        2.0 / (grid_size * grid_size)
    )
    prev_real = previous[:, 0]
    prev_imag = previous[:, 1]
    sub_piece = lax.all_gather(subspace, "band", axis=0, tiled=True)
    sub_real = sub_piece[:, 0]
    sub_imag = sub_piece[:, 1]
    over_real = jnp.einsum(
        "jg,ig->ji", sub_real, prev_real, preferred_element_type=jnp.float32
    ) + jnp.einsum("jg,ig->ji", sub_imag, prev_imag, preferred_element_type=jnp.float32)
    over_imag = jnp.einsum(
        "jg,ig->ji", sub_real, prev_imag, preferred_element_type=jnp.float32
    ) - jnp.einsum("jg,ig->ji", sub_imag, prev_real, preferred_element_type=jnp.float32)
    partial_value = jnp.stack([over_real, over_imag])
    intersection = lax.psum_scatter(partial_value, "fft", scatter_dimension=1, tiled=True)
    stick_buffer = jnp.einsum(
        "bpi,zi,si->bpzs", orbitals, plane_hot, stick_hot, preferred_element_type=jnp.float32
    ).astype(jnp.bfloat16)

    def potential_work(along_y):
        along_x = apply_dft(along_y[0], along_y[1], forward, "zxy,xk->zky")
        weighted = packed((along_x[0] * potential, along_x[1] * potential), 0)
        back_x = packed(apply_dft(weighted[0], weighted[1], inverse, "zxy,xk->zky"), 0)
        return packed(apply_dft(back_x[0], back_x[1], inverse, "zxy,yk->zxk"), 0)

    along_z = packed(apply_dft(stick_buffer[:, 0], stick_buffer[:, 1], forward, "bzs,zk->bks"), 1)
    all_columns = lax.all_gather(stick_column, "fft", axis=0, tiled=True)
    owners = all_columns.shape[0] // stick_count
    block_columns = (all_columns % slab_cells).reshape(owners, stick_count)
    block_hot = (
        block_columns[:, :, None] == jnp.arange(slab_cells, dtype=jnp.int32)[None, None, :]
    ).astype(jnp.bfloat16)

    def stick_work(one_band):
        plane_depth = one_band.shape[1]
        split_band = one_band.reshape(2, plane_depth, owners, stick_count)
        plane_grid = jnp.einsum(
            "pzds,dsc->pzdc", split_band, block_hot, preferred_element_type=jnp.float32
        ).astype(jnp.bfloat16)
        plane_grid = plane_grid.reshape(2, plane_depth, grid_size, grid_size)
        along_y = packed(apply_dft(plane_grid[0], plane_grid[1], forward, "zxy,yk->zxk"), 0)
        back_y = potential_work(along_y)
        back_split = back_y.reshape(2, plane_depth, owners, slab_cells)
        picked = jnp.einsum(
            "pzdc,dsc->pzds", back_split, block_hot, preferred_element_type=jnp.float32
        ).astype(jnp.bfloat16)
        return picked.reshape(2, plane_depth, owners * stick_count)

    finished = lax.map(
        stick_work, lax.all_to_all(along_z, "fft", split_axis=2, concat_axis=3, tiled=True)
    )
    stick_values = lax.all_to_all(finished, "fft", split_axis=3, concat_axis=2, tiled=True)
    picked_sticks = jnp.einsum(
        "bpzs,si->bpzi", stick_values, stick_hot, preferred_element_type=jnp.float32
    ).astype(jnp.bfloat16)
    cosine_cols = jnp.einsum("zk,ki->zi", inverse[0], plane_hot, preferred_element_type=jnp.float32)
    sine_cols = jnp.einsum("zk,ki->zi", inverse[1], plane_hot, preferred_element_type=jnp.float32)
    pick_real = picked_sticks[:, 0].astype(jnp.float32)
    pick_imag = picked_sticks[:, 1].astype(jnp.float32)
    wave_real = jnp.sum(pick_real * cosine_cols[None] - pick_imag * sine_cols[None], axis=1)
    wave_imag = jnp.sum(pick_real * sine_cols[None] + pick_imag * cosine_cols[None], axis=1)
    real_out = wave_real + kinetic * orbitals[:, 0].astype(jnp.float32)
    imag_out = wave_imag + kinetic * orbitals[:, 1].astype(jnp.float32)
    applied = jnp.stack([real_out, imag_out], axis=1).astype(jnp.bfloat16)
    return (applied, intersection)


PLANES = 4
PAIR = 2
LANES = 128
CHUNK = 4 * PLANES
EXTRA = 16


def phases(products, length):
    angle = (products % length).astype(np.float64) * (2.0 * np.pi / length)
    return np.cos(angle), np.sin(angle)


def as_bf16(array):
    return jnp.asarray(array, jnp.bfloat16)


def line_tables(length):
    cosine, sine = phases(np.outer(np.arange(length), np.arange(length)), length)

    def spread(table):
        rest = table[:, LANES:]
        return table[:, :LANES], np.concatenate([rest, rest], axis=1)

    tables = []
    for to_real, to_imag in ((cosine, sine), (-sine, cosine)):
        real_main, real_rest = spread(to_real)
        imag_main, imag_rest = spread(to_imag)
        tables.append(np.concatenate([real_main, imag_main, real_rest, imag_rest], axis=1))
    there = np.stack(tables)
    return as_bf16(there), as_bf16(there.transpose(0, 2, 1))


def half_tables(length):
    half = np.arange(length // 2)
    natural = np.arange(length).reshape(2, length // 16, 8)
    mixed = natural.transpose(1, 0, 2).reshape(-1)
    there, back = [], []
    for parity in (0, 1):
        cosine, sine = phases(np.outer(2 * half + parity, half), length)
        table = np.block([[cosine, -sine], [sine, cosine]])
        there.append(table[:, mixed])
        back.append(table.T)
    return as_bf16(np.stack(there + back))


def column_tables(length, slab):
    cosine, sine = phases(np.outer(np.arange(length), np.arange(length)), length)
    table = np.block([[cosine, -sine], [sine, cosine]])
    order = np.arange(2 * length).reshape(2, length // slab, slab // PLANES, PLANES)
    order = order.transpose(2, 1, 0, 3).reshape(-1)
    there = table[order]
    return as_bf16(there), as_bf16(there.T)


def pick_table(slab):
    lines = PLANES * PAIR
    table = np.zeros((CHUNK, lines * slab))
    for plane in range(PLANES):
        for band in range(PAIR):
            line = plane * PAIR + band
            for part in range(2):
                row = band * 2 * PLANES + part * PLANES + plane
                table[row, line * slab : (line + 1) * slab] = 1.0
    return as_bf16(table)


def whole_kernel(
    mesh_bands,
    orbital_ref,
    slot_ref,
    column_ref,
    previous_ref,
    subspace_hbm,
    pot_ref,
    deep_hbm,
    rise_hbm,
    line_hbm,
    turn_hbm,
    half_hbm,
    pick_ref,
    applied_ref,
    inter_ref,
    subspace_ref,
    deep_ref,
    rise_ref,
    line_ref,
    turn_ref,
    half_ref,
    full_ref,
    left_ref,
    right_ref,
    wave_ref,
    found_ref,
    kinetic_ref,
    hot_ref,
    gather_ref,
    sent_ref,
    stick_ref,
    coord_ref,
    coords_ref,
    mask_ref,
    there_ref,
    again_ref,
    mixed_ref,
    heavy_ref,
    after_ref,
    kept_ref,
    stage_ref,
    back_ref,
    every_ref,
    right_side_ref,
    share_ref,
    shares_ref,
    load_sem,
    send_sem,
    recv_sem,
    home_send,
    home_recv,
    coord_send,
    coord_recv,
    band_send,
    band_recv,
    share_send,
    share_recv,
):
    slab, size, _ = pot_ref.shape
    owners = size // slab
    half_owners = owners // 2
    half = size // 2
    groups_pair = slab // PLANES
    waves = slot_ref.shape[1]
    blocks = waves // LANES
    sticks = LANES
    lines = PLANES * PAIR
    bands = orbital_ref.shape[0]
    pairs = bands // PAIR
    groups = pairs * groups_pair
    rest = size - LANES
    scale = 1.0 / (size * size)
    mine = subspace_ref.shape[0]
    share = share_ref.shape[1]
    shares = mine // share
    me = lax.axis_index("fft")
    band_me = lax.axis_index("band")
    every_band = [lax.rem(band_me + shift, mesh_bands) for shift in range(mesh_bands)]
    others = [lax.rem(me + shift, owners) for shift in range(1, owners)]
    f32, bf16 = jnp.float32, jnp.bfloat16

    def dot(left, right):
        return jnp.dot(left, right, preferred_element_type=f32)

    def remote(src, dst, send, recv, target):
        return pltpu.make_async_remote_copy(
            src_ref=src,
            dst_ref=dst,
            send_sem=send,
            recv_sem=recv,
            device_id=target,
            device_id_type=pl.DeviceIdType.MESH,
        )

    def coord_copy(place):
        return remote(
            coord_ref,
            coords_ref.at[me],
            coord_send.at[place],
            coord_recv.at[place],
            {"fft": others[place]},
        )

    def band_copy(place):
        return remote(
            previous_ref,
            every_ref.at[band_me],
            band_send.at[place],
            band_recv.at[place],
            {"band": every_band[place + 1]},
        )

    def share_copy(block, place):
        return remote(
            share_ref.at[block],
            shares_ref.at[me],
            share_send.at[block, place],
            share_recv.at[me],
            {"band": every_band[place], "fft": shares * band_me + block},
        )

    def share_arrival(source):
        return remote(
            share_ref.at[0],
            shares_ref.at[source],
            share_send.at[0, 0],
            share_recv.at[source],
            {"fft": others[0]},
        )

    def there_copy(group, place):
        return remote(
            sent_ref.at[group, others[place]],
            stick_ref.at[group, me],
            send_sem.at[group, place],
            recv_sem.at[group, place],
            {"fft": others[place]},
        )

    def home_copy(group, place):
        return remote(
            stage_ref.at[group + 2, others[place]],
            back_ref.at[group, me],
            home_send.at[group, place],
            home_recv.at[group, place],
            {"fft": others[place]},
        )

    loads = []
    for place, (src, dst) in enumerate(
        (
            (deep_hbm, deep_ref),
            (line_hbm, line_ref),
            (turn_hbm, turn_ref),
            (subspace_hbm, subspace_ref),
            (pot_ref, full_ref),
            (pot_ref.at[:, :, :LANES], left_ref),
            (half_hbm, half_ref),
            (rise_hbm, rise_ref),
        )
    ):
        loads.append(pltpu.make_async_copy(src, dst, load_sem.at[place]))
        loads[-1].start()

    barrier = pltpu.get_barrier_semaphore()
    for place in range(mesh_bands):
        for other in [me] + others:
            if place or other is not me:
                pl.semaphore_signal(
                    barrier,
                    inc=1,
                    device_id={"band": every_band[place], "fft": other},
                    device_id_type=pl.DeviceIdType.MESH,
                )

    low_lane = lax.broadcasted_iota(jnp.int32, (1, LANES), 1) < rest
    level = lax.broadcasted_iota(jnp.int32, (half, LANES), 0)
    wave_ref[...] = orbital_ref[...].reshape(2 * bands, waves).astype(f32)

    column = column_ref[...]
    grid_x = jnp.floor((column.astype(f32) + 0.5) * (1.0 / size))
    grid_y = column.astype(f32) - grid_x * size
    coord_row = lax.broadcasted_iota(jnp.int32, (8, LANES), 0)
    first_x = lax.convert_element_type(me * slab, f32)
    coord_ref[...] = jnp.where(coord_row == 0, grid_x - first_x, jnp.where(coord_row == 1, grid_y, 0.0))

    def lanes_of(block, count=1):
        return pl.ds(pl.multiple_of(block * LANES, LANES), count * LANES)

    def plane_of(block):
        return lax.shift_right_logical(slot_ref[:, lanes_of(block)], 7)

    @pl.loop(0, blocks, unroll=4)
    def _(block):
        slot = slot_ref[:, lanes_of(block)]
        cell = jnp.where(plane_of(block) >= half, sticks, 0) + jnp.bitwise_and(slot, sticks - 1)
        rows = lax.broadcasted_iota(jnp.int32, (2 * sticks, LANES), 0)
        hot_ref[:, lanes_of(block)] = jnp.where(cell == rows, 1.0, 0.0).astype(bf16)

    pl.semaphore_wait(barrier, mesh_bands * owners - 1)
    for place in range(owners - 1):
        coord_copy(place).start()
    for place in range(mesh_bands - 1):
        band_copy(place).start()
    coords_ref[me] = coord_ref[...]
    every_ref[band_me] = previous_ref[...]

    def level_mask(block):
        plane = plane_of(block)
        return jnp.where(plane >= half, plane - half, plane) == level

    def scatter_waves(pair):
        cells = None
        for block in range(0, blocks, 2):
            pieces = []
            for step in range(2):
                chosen = level_mask(block + step)
                values = wave_ref[
                    2 * PAIR * pair : 2 * PAIR * (pair + 1), lanes_of(block + step)
                ]
                rows = []
                for part in range(2 * PAIR):
                    rows.append(jnp.where(chosen, values[part : part + 1], 0.0))
                pieces.append(jnp.concatenate(rows, axis=0))
            left = jnp.concatenate(pieces, axis=1).astype(bf16)
            term = lax.dot_general(
                left,
                hot_ref[:, lanes_of(block, 2)],
                (((1,), (1,)), ((), ())),
                preferred_element_type=f32,
            )
            cells = term if cells is None else cells + term
        columns = []
        for band in range(PAIR):
            pieces = []
            for part in range(2):
                start = (2 * band + part) * half
                for side in range(2):
                    pieces.append(cells[start : start + half, side * LANES : (side + 1) * LANES])
            columns.append(jnp.concatenate(pieces, axis=0))
        columns = jnp.concatenate(columns, axis=1).astype(bf16)
        if pair == 0:
            loads[0].wait()
        along = dot(deep_ref[...], columns).reshape(groups_pair * owners, 2 * PLANES, PAIR * LANES)
        chunks = jnp.concatenate([along[:, :, :LANES], along[:, :, LANES:]], axis=1)
        first = pair * groups_pair
        sent_ref[first : first + groups_pair] = chunks.astype(bf16).reshape(
            groups_pair, owners, CHUNK, LANES
        )

        @pl.loop(0, groups_pair)
        def _(step):
            for place in range(owners - 1):
                there_copy(first + step, place).start()
            stick_ref[first + step, me] = sent_ref[first + step, me]

    for pair in range(pairs):
        scatter_waves(pair)

    freq_x = jnp.where(grid_x >= half, grid_x - size, grid_x)
    freq_y = jnp.where(grid_y >= half, grid_y - size, grid_y)
    freq_row = lax.broadcasted_iota(jnp.int32, (16, LANES), 0)
    freqs = jnp.where(freq_row == 0, freq_x, jnp.where(freq_row == 1, freq_y, 0.0))
    freqs = jnp.concatenate([freqs, freqs], axis=1).astype(bf16)

    @pl.loop(0, blocks // 8)
    def _(step):
        found = dot(freqs, hot_ref[:, lanes_of(8 * step, 8)])
        plane = lax.shift_right_logical(slot_ref[:, lanes_of(8 * step, 8)], 7)
        freq_z = jnp.where(plane >= half, plane - size, plane).astype(f32)
        total = freq_z * freq_z + found[0:1] * found[0:1] + found[1:2] * found[1:2]
        kinetic_ref[:, lanes_of(8 * step, 8)] = total * (2.0 / (size * size))

    for place in range(1, len(loads)):
        loads[place].wait()

    @pl.loop(0, slab)
    def _(plane):
        local = full_ref[plane, :, LANES:]
        right_ref[plane] = jnp.concatenate([local, local], axis=1)

    for place in range(owners - 1):
        coord_copy(place).wait()

    @pl.loop(0, owners)
    def _(owner):
        coords = coords_ref[owner]
        local = lax.broadcasted_iota(jnp.int32, (slab, sticks), 0).astype(f32)
        mask_ref[owner] = jnp.where(coords[0:1, :] == local, 1.0, 0.0)
        cells = lax.broadcasted_iota(jnp.int32, (size, sticks), 0).astype(f32)
        hot = jnp.where(coords[1:2, :] == cells, 1.0, 0.0).astype(bf16)
        for part in range(2):
            rows = lax.dot_general(
                hot, line_ref[part], (((0,), (0,)), ((), ())), preferred_element_type=f32
            )
            there_ref[owner, part * sticks : (part + 1) * sticks, :] = rows.astype(bf16)
            turned = dot(turn_ref[part], hot)
            again_ref[owner, :, part * sticks : (part + 1) * sticks] = turned.astype(bf16)

    for place in range(mesh_bands - 1):
        band_copy(place).wait()

    count = mesh_bands * bands
    others_side = every_ref[...].reshape(count, 2, waves).astype(f32)
    right_side_ref[:count] = others_side[:, 0].astype(bf16)
    right_side_ref[count : 2 * count] = others_side[:, 1].astype(bf16)
    own_side = subspace_ref[...].astype(f32)
    own_side = jnp.concatenate([own_side[:, 0], own_side[:, 1]], axis=0).astype(bf16)
    products = lax.dot_general(
        own_side, right_side_ref[...], (((1,), (1,)), ((), ())), preferred_element_type=f32
    )
    lane = lax.broadcasted_iota(jnp.int32, (1, LANES), 1)
    upper, lower = products[:mine], products[mine:]
    blend = jnp.where(
        lane < count,
        upper + pltpu.roll(lower, LANES - count, 1),
        upper - pltpu.roll(lower, count, 1),
    )
    for block in range(shares):
        share_ref[block] = blend[block * share : (block + 1) * share]

    source_band = lax.div(me, shares)
    for block in range(shares):
        for place in range(mesh_bands):
            if place:
                share_copy(block, place).start()
            else:
                to_self = shares * band_me + block == me

                @pl.when(jnp.logical_not(to_self))
                def _():
                    share_copy(block, place).start()

                @pl.when(to_self)
                def _():
                    shares_ref[me] = share_ref[block]

    def spread_lines(group):
        for low in range(half_owners):
            results = []
            for owner in (low, low + half_owners):
                values = stick_ref[group, owner].astype(f32)
                mask = mask_ref[owner]
                parts = []
                for part in range(2):
                    pieces = []
                    for plane in range(PLANES):
                        for band in range(PAIR):
                            row = band * 2 * PLANES + part * PLANES + plane
                            pieces.append(values[row : row + 1, :] * mask)
                    parts.append(jnp.concatenate(pieces, axis=0))
                left = jnp.concatenate(parts, axis=1).astype(bf16)
                results.append(dot(left, there_ref[owner]))
            for plane in range(PLANES):
                unit, side = plane // 2, plane % 2
                start = plane * PAIR * slab

                def pieces_of(result):
                    one = result[start : start + slab]
                    two = result[start + slab : start + 2 * slab]
                    found = []
                    for half_lines in (one, two):
                        found.append((half_lines[:, :LANES], half_lines[:, LANES : 2 * LANES]))
                    both = []
                    for offset in (2 * LANES, 3 * LANES):
                        both.append(
                            jnp.where(
                                low_lane,
                                one[:, offset : offset + LANES],
                                two[:, offset : offset + LANES],
                            )
                        )
                    found.append(tuple(both))
                    return found

                near, far = pieces_of(results[0]), pieces_of(results[1])
                offsets = (2 * side * LANES, (2 * side + 1) * LANES, (4 + side) * LANES)
                for (near_re, near_im), (far_re, far_im), offset in zip(near, far, offsets):
                    for parity in range(2):
                        if parity == 0:
                            real, imag = near_re + far_re, near_im + far_im
                        else:
                            real, imag = near_re - far_re, near_im - far_im
                        tile = jnp.concatenate(
                            [real.reshape(-1, 8, LANES), imag.reshape(-1, 8, LANES)], axis=1
                        )
                        mixed_ref[
                            unit,
                            parity,
                            slice(2 * slab * low, 2 * slab * (low + 1)),
                            offset : offset + LANES,
                        ] = tile.reshape(2 * slab, LANES).astype(bf16)

    def forward_lines(group, unit):
        first = lax.rem(group, groups_pair) * PLANES
        if True:
            for parity in range(2):
                picks = pl.ds(parity, half, 2)

                for tile in range(3):
                    result = dot(
                        half_ref[parity],
                        mixed_ref[unit, parity, :, 2 * LANES * tile : 2 * LANES * (tile + 1)],
                    )
                    if tile < 2:
                        local = left_ref[first + 2 * unit + tile, picks, :]
                        local = jnp.concatenate([local, local], axis=1)
                    else:
                        one = right_ref[first + 2 * unit, picks, :]
                        two = right_ref[first + 2 * unit + 1, picks, :]
                        local = jnp.concatenate([one, two], axis=1)
                    heavy_ref[unit, parity, tile, :half] = (result[:half] * local).astype(bf16)
                    heavy_ref[unit, parity, tile, half:] = (result[half:] * local).astype(bf16)

    def backward_lines(unit):
        if True:
            for tile in range(3):
                even = dot(half_ref[2], heavy_ref[unit, 0, tile])
                odd = dot(half_ref[3], heavy_ref[unit, 1, tile])
                for side, values in enumerate((even + odd, even - odd)):
                    for low in range(half_owners):
                        owner = low + side * half_owners
                        for part in range(2):
                            start = part * half + low * slab
                            found = values[start : start + slab]
                            one, two = found[:, :LANES], found[:, LANES:]
                            if tile < 2:
                                rows = pl.ds(
                                    pl.multiple_of((2 * unit + tile) * 2 * slab, 2 * slab), 2 * slab
                                )
                                after_ref[owner, rows, part * LANES : (part + 1) * LANES] = (
                                    jnp.concatenate([one, two], axis=0).astype(bf16)
                                )
                            else:
                                for place, both in enumerate((one, two)):
                                    plane = 2 * unit + place
                                    rows = pl.ds(
                                        pl.multiple_of(plane * 2 * slab, 2 * slab), 2 * slab
                                    )
                                    after_ref[
                                        owner, rows, (2 + part) * LANES : (3 + part) * LANES
                                    ] = jnp.concatenate(
                                        [
                                            jnp.where(low_lane, both, 0.0),
                                            jnp.where(low_lane, 0.0, both),
                                        ],
                                        axis=0,
                                    ).astype(bf16)

    part_row = lax.broadcasted_iota(jnp.int32, (CHUNK, LANES), 0)
    part_row = jnp.bitwise_and(part_row, PLANES) == 0

    def weighed_lines():
        for owner in range(owners):
            result = dot(after_ref[owner], again_ref[owner])
            mask = mask_ref[owner] * scale
            mask = jnp.concatenate([mask, mask], axis=1)[None]
            kept = (result.reshape(lines, slab, 2 * LANES) * mask).reshape(lines * slab, 2 * LANES)
            kept_ref[owner] = kept.astype(bf16)

    def picked_lines(place):
        for owner in range(owners):
            found = dot(pick_ref[...], kept_ref[owner])
            stage_ref[place, owner] = jnp.where(
                part_row, found[:, :LANES], found[:, LANES:]
            ).astype(bf16)

    def wait_group(group):
        for place in range(owners - 1):
            there_copy(group, place).wait()

    def send_home(group):
        for place in range(owners - 1):
            home_copy(group, place).start()
        back_ref[group, me] = stage_ref[group + 2, me]

    wait_group(0)
    spread_lines(0)

    @pl.loop(0, groups)
    def _(group):
        @pl.when(group < groups - 1)
        def _():
            wait_group(group + 1)

        forward_lines(group, 0)
        forward_lines(group, 1)
        picked_lines(group)
        weighed_lines()
        backward_lines(0)
        backward_lines(1)
        spread_lines(lax.rem(group + 1, groups))

        @pl.when(group > 1)
        def _():
            send_home(group - 2)

    picked_lines(groups)
    weighed_lines()
    send_home(groups - 2)
    picked_lines(groups + 1)
    send_home(groups - 1)

    def gather_waves(pair):
        first = pair * groups_pair

        @pl.loop(0, groups_pair)
        def _(step):
            for place in range(owners - 1):
                home_copy(first + step, place).wait()

        chunks = back_ref[first : first + groups_pair].reshape(groups_pair * owners, CHUNK, LANES)
        chunks = chunks.astype(f32)
        columns = []
        for band in range(PAIR):
            rows = chunks[:, band * 2 * PLANES : (band + 1) * 2 * PLANES]
            columns.append(rows.reshape(2 * size, LANES))
        columns = jnp.concatenate(columns, axis=1).astype(bf16)
        risen = (dot(rise_ref[...], columns) * (1.0 / size)).astype(bf16)
        pieces = []
        for band in range(PAIR):
            for part in range(2):
                both = []
                for side in range(2):
                    start = part * size + side * half
                    both.append(risen[start : start + half, band * LANES : (band + 1) * LANES])
                pieces.append(jnp.concatenate(both, axis=1))
        gather_ref[...] = jnp.concatenate(pieces, axis=0)

        @pl.loop(0, blocks // 2, unroll=4)
        def _(step):
            values = dot(gather_ref[...], hot_ref[:, lanes_of(2 * step, 2)])
            for side in range(2):
                chosen = level_mask(2 * step + side)
                for part in range(2 * PAIR):
                    ours = values[part * half : (part + 1) * half, side * LANES : (side + 1) * LANES]
                    row = 2 * PAIR * pair + part
                    found_ref[row : row + 1, lanes_of(2 * step + side)] = jnp.sum(
                        jnp.where(chosen, ours, 0.0), axis=0, keepdims=True
                    )

    for pair in range(pairs):
        gather_waves(pair)

    result = found_ref[...] + kinetic_ref[...] * wave_ref[...]
    applied_ref[...] = result.astype(bf16).reshape(bands, 2, waves)

    for block in range(shares):
        for place in range(mesh_bands):
            if place:
                share_copy(block, place).wait_send()
            else:

                @pl.when(shares * band_me + block != me)
                def _():
                    share_copy(block, place).wait_send()

    for source in range(owners):
        from_self = jnp.logical_and(source_band == band_me, me == source)

        @pl.when(jnp.logical_not(from_self))
        def _():
            share_arrival(source).wait_recv()

    total = shares_ref[0]
    for source in range(1, owners):
        total = total + shares_ref[source]
    total = pltpu.roll(total, lax.rem(LANES - bands * band_me, LANES), 1)
    inter_ref[0] = total[:, :bands]
    inter_ref[1] = total[:, count : count + bands]


def whole_work(mesh_bands, orbitals, slots, columns, potential, subspace, previous):
    slab, size, _ = potential.shape
    owners = size // slab
    groups_pair = slab // PLANES
    bands, _, waves = orbitals.shape
    groups = bands // PAIR * groups_pair
    half = size // 2
    lines = PLANES * PAIR
    mine = subspace.shape[0]
    share = mine * mesh_bands // owners
    deep, rise = column_tables(size, slab)
    line, turn = line_tables(size)
    halves = half_tables(size)
    pick = pick_table(slab)
    in_vmem = pl.BlockSpec(memory_space=pltpu.VMEM)
    anywhere = pl.BlockSpec(memory_space=pl.ANY)
    bf16, f32 = jnp.bfloat16, jnp.float32
    dma = pltpu.SemaphoreType.DMA
    return pl.pallas_call(
        functools.partial(whole_kernel, mesh_bands),
        out_shape=(
            jax.ShapeDtypeStruct(orbitals.shape, bf16),
            jax.ShapeDtypeStruct((2, share, bands), f32),
        ),
        in_specs=[in_vmem] * 4 + [anywhere] * 7 + [in_vmem],
        out_specs=(in_vmem, in_vmem),
        scratch_shapes=[
            pltpu.VMEM(subspace.shape, bf16),
            pltpu.VMEM(deep.shape, bf16),
            pltpu.VMEM(rise.shape, bf16),
            pltpu.VMEM(line.shape, bf16),
            pltpu.VMEM(turn.shape, bf16),
            pltpu.VMEM(halves.shape, bf16),
            pltpu.VMEM((slab, size, size), f32),
            pltpu.VMEM((slab, size, LANES), f32),
            pltpu.VMEM((slab, size, LANES), f32),
            pltpu.VMEM((2 * bands, waves), f32),
            pltpu.VMEM((2 * bands, waves), f32),
            pltpu.VMEM((1, waves), f32),
            pltpu.VMEM((2 * LANES, waves), bf16),
            pltpu.VMEM((2 * PAIR * half, 2 * LANES), bf16),
            pltpu.VMEM((groups, owners, CHUNK, LANES), bf16),
            pltpu.VMEM((groups, owners, CHUNK, LANES), bf16),
            pltpu.VMEM((8, LANES), f32),
            pltpu.VMEM((owners, 8, LANES), f32),
            pltpu.VMEM((owners, slab, LANES), f32),
            pltpu.VMEM((owners, 2 * LANES, 4 * LANES), bf16),
            pltpu.VMEM((owners, 4 * LANES, 2 * LANES), bf16),
            pltpu.VMEM((PLANES // 2, 2, size, 6 * LANES), bf16),
            pltpu.VMEM((PLANES // 2, 2, 3, size, 2 * LANES), bf16),
            pltpu.VMEM((owners, lines * slab, 4 * LANES), bf16),
            pltpu.VMEM((owners, lines * slab, 2 * LANES), bf16),
            pltpu.VMEM((groups + 2, owners, CHUNK, LANES), bf16),
            pltpu.VMEM((groups, owners, CHUNK, LANES), bf16),
            pltpu.VMEM((mesh_bands, bands, 2, waves), bf16),
            pltpu.VMEM((LANES, waves), bf16),
            pltpu.VMEM((mine // share, share, LANES), f32),
            pltpu.VMEM((owners, share, LANES), f32),
            dma((8,)),
            dma((groups, owners - 1)),
            dma((groups, owners - 1)),
            dma((groups, owners - 1)),
            dma((groups, owners - 1)),
            dma((owners - 1,)),
            dma((owners - 1,)),
            dma((mesh_bands - 1,)),
            dma((mesh_bands - 1,)),
            dma((mine // share, mesh_bands)),
            dma((owners,)),
        ],
        compiler_params=pltpu.CompilerParams(
            collective_id=0, has_side_effects=True, vmem_limit_bytes=60 * 1024 * 1024
        ),
        cost_estimate=pl.CostEstimate(
            flops=40 * 10**9, bytes_accessed=8 * 10**6, transcendentals=0
        ),
    )(
        orbitals,
        slots,
        columns,
        previous,
        subspace,
        potential,
        deep,
        rise,
        line,
        turn,
        halves,
        pick,
    )


def fast_device(mesh_bands, orbitals, sphere_slot, stick_column, potential, subspace, previous):
    slots = sphere_slot.reshape(1, -1)
    columns = stick_column.reshape(1, -1)
    return whole_work(mesh_bands, orbitals, slots, columns, potential, subspace, previous)


def fits(mesh_bands, orbitals, slots, sticks, potential, subspace, previous):
    slab, size, _ = potential.shape
    owners = size // slab
    bands, mine = orbitals.shape[0], subspace.shape[0]
    good = slab % 8 == 0 and owners % 2 == 0 and owners * slab == size
    good = good and 2 * size == 3 * LANES and sticks.shape[0] == LANES
    good = good and bands % PAIR == 0 and slots.shape[0] % (8 * LANES) == 0
    good = good and mine * mesh_bands % (8 * owners) == 0 and owners % mesh_bands == 0
    return good and 2 * mesh_bands * bands <= LANES


def per_device(mesh_bands, *arrays):
    if fits(mesh_bands, *arrays):
        return fast_device(mesh_bands, *arrays)
    return general_device(*arrays)


def solution(mesh):
    return jax.shard_map(
        functools.partial(per_device, mesh.shape["band"]),
        mesh=mesh,
        in_specs=(
            P("band", None, "fft"),
            P("fft"),
            P("fft"),
            P("fft", None, None),
            P("band", None, "fft"),
            P("band", None, "fft"),
        ),
        out_specs=(P("band", None, "fft"), P(None, "fft", "band")),
        check_vma=False,
    )
```

```python
import functools
import math

import jax
import jax.numpy as jnp
import numpy as np
from jax import lax
from jax.experimental import pallas as pl
from jax.experimental.pallas import tpu as pltpu
from jax.sharding import PartitionSpec as P


def dft_table(length, sign_value, factor):
    positions = jnp.arange(length, dtype=jnp.int32)
    phase_step = positions[:, None] * positions[None, :] % length
    angle_value = phase_step.astype(jnp.float32) * (2.0 * math.pi / length)
    cosine = (jnp.cos(angle_value) * factor).astype(jnp.bfloat16)
    sine_part = (jnp.sin(angle_value) * (sign_value * factor)).astype(jnp.bfloat16)
    return (cosine, sine_part)


def apply_dft(real_in, imag_in, table, form):
    cosine, sine_part = table

    def product(operand, table_part):
        return jnp.einsum(form, operand, table_part, preferred_element_type=jnp.float32)

    real_out = product(real_in, cosine) - product(imag_in, sine_part)
    imag_out = product(real_in, sine_part) + product(imag_in, cosine)
    return (real_out, imag_out)


def packed(pair, axis_pos):
    return jnp.stack([pair[0].astype(jnp.bfloat16), pair[1].astype(jnp.bfloat16)], axis=axis_pos)


def frequency(values, grid_size):
    return jnp.where(values >= grid_size // 2, values - grid_size, values).astype(jnp.float32)


def one_hot_rows(indices, count):
    return (indices[None, :] == jnp.arange(count, dtype=jnp.int32)[:, None]).astype(jnp.bfloat16)


def general_device(orbitals, sphere_slot, stick_column, potential, subspace, previous):
    slab_depth = potential.shape[0]
    grid_size = potential.shape[1]
    stick_count = stick_column.shape[0]
    slab_cells = slab_depth * grid_size
    forward = dft_table(grid_size, 1.0, 1.0)
    inverse = dft_table(grid_size, -1.0, 1.0 / grid_size)
    plane_index = sphere_slot // stick_count
    stick_index = sphere_slot % stick_count
    plane_hot = one_hot_rows(plane_index, grid_size)
    stick_hot = one_hot_rows(stick_index, stick_count)
    stick_coords = jnp.stack([stick_column // grid_size, stick_column % grid_size]).astype(
        jnp.bfloat16
    )
    wave_coords = jnp.dot(stick_coords, stick_hot, preferred_element_type=jnp.float32)
    freq_z = frequency(plane_index, grid_size)
    freq_x = frequency(wave_coords[0].astype(jnp.int32), grid_size)
    freq_y = frequency(wave_coords[1].astype(jnp.int32), grid_size)
    kinetic = (freq_z * freq_z + freq_x * freq_x + freq_y * freq_y) * (
        2.0 / (grid_size * grid_size)
    )
    prev_real = previous[:, 0]
    prev_imag = previous[:, 1]
    sub_piece = lax.all_gather(subspace, "band", axis=0, tiled=True)
    sub_real = sub_piece[:, 0]
    sub_imag = sub_piece[:, 1]
    over_real = jnp.einsum(
        "jg,ig->ji", sub_real, prev_real, preferred_element_type=jnp.float32
    ) + jnp.einsum("jg,ig->ji", sub_imag, prev_imag, preferred_element_type=jnp.float32)
    over_imag = jnp.einsum(
        "jg,ig->ji", sub_real, prev_imag, preferred_element_type=jnp.float32
    ) - jnp.einsum("jg,ig->ji", sub_imag, prev_real, preferred_element_type=jnp.float32)
    partial_value = jnp.stack([over_real, over_imag])
    intersection = lax.psum_scatter(partial_value, "fft", scatter_dimension=1, tiled=True)
    stick_buffer = jnp.einsum(
        "bpi,zi,si->bpzs", orbitals, plane_hot, stick_hot, preferred_element_type=jnp.float32
    ).astype(jnp.bfloat16)

    def potential_work(along_y):
        along_x = apply_dft(along_y[0], along_y[1], forward, "zxy,xk->zky")
        weighted = packed((along_x[0] * potential, along_x[1] * potential), 0)
        back_x = packed(apply_dft(weighted[0], weighted[1], inverse, "zxy,xk->zky"), 0)
        return packed(apply_dft(back_x[0], back_x[1], inverse, "zxy,yk->zxk"), 0)

    along_z = packed(apply_dft(stick_buffer[:, 0], stick_buffer[:, 1], forward, "bzs,zk->bks"), 1)
    all_columns = lax.all_gather(stick_column, "fft", axis=0, tiled=True)
    owners = all_columns.shape[0] // stick_count
    block_columns = (all_columns % slab_cells).reshape(owners, stick_count)
    block_hot = (
        block_columns[:, :, None] == jnp.arange(slab_cells, dtype=jnp.int32)[None, None, :]
    ).astype(jnp.bfloat16)

    def stick_work(one_band):
        plane_depth = one_band.shape[1]
        split_band = one_band.reshape(2, plane_depth, owners, stick_count)
        plane_grid = jnp.einsum(
            "pzds,dsc->pzdc", split_band, block_hot, preferred_element_type=jnp.float32
        ).astype(jnp.bfloat16)
        plane_grid = plane_grid.reshape(2, plane_depth, grid_size, grid_size)
        along_y = packed(apply_dft(plane_grid[0], plane_grid[1], forward, "zxy,yk->zxk"), 0)
        back_y = potential_work(along_y)
        back_split = back_y.reshape(2, plane_depth, owners, slab_cells)
        picked = jnp.einsum(
            "pzdc,dsc->pzds", back_split, block_hot, preferred_element_type=jnp.float32
        ).astype(jnp.bfloat16)
        return picked.reshape(2, plane_depth, owners * stick_count)

    finished = lax.map(
        stick_work, lax.all_to_all(along_z, "fft", split_axis=2, concat_axis=3, tiled=True)
    )
    stick_values = lax.all_to_all(finished, "fft", split_axis=3, concat_axis=2, tiled=True)
    picked_sticks = jnp.einsum(
        "bpzs,si->bpzi", stick_values, stick_hot, preferred_element_type=jnp.float32
    ).astype(jnp.bfloat16)
    cosine_cols = jnp.einsum("zk,ki->zi", inverse[0], plane_hot, preferred_element_type=jnp.float32)
    sine_cols = jnp.einsum("zk,ki->zi", inverse[1], plane_hot, preferred_element_type=jnp.float32)
    pick_real = picked_sticks[:, 0].astype(jnp.float32)
    pick_imag = picked_sticks[:, 1].astype(jnp.float32)
    wave_real = jnp.sum(pick_real * cosine_cols[None] - pick_imag * sine_cols[None], axis=1)
    wave_imag = jnp.sum(pick_real * sine_cols[None] + pick_imag * cosine_cols[None], axis=1)
    real_out = wave_real + kinetic * orbitals[:, 0].astype(jnp.float32)
    imag_out = wave_imag + kinetic * orbitals[:, 1].astype(jnp.float32)
    applied = jnp.stack([real_out, imag_out], axis=1).astype(jnp.bfloat16)
    return (applied, intersection)


PLANES = 4
PAIR = 2
LANES = 128
CHUNK = 4 * PLANES
FOLD = 4


def phases(products, length):
    angle = (products % length).astype(np.float64) * (2.0 * np.pi / length)
    return np.cos(angle), np.sin(angle)


def as_bf16(array):
    return jnp.asarray(array, jnp.bfloat16)


def line_tables(length):
    cosine, sine = phases(np.outer(np.arange(length), np.arange(length)), length)

    def spread(table):
        rest = table[:, LANES:]
        return table[:, :LANES], np.concatenate([rest, rest], axis=1)

    tables = []
    for to_real, to_imag in ((cosine, sine), (-sine, cosine)):
        real_main, real_rest = spread(to_real)
        imag_main, imag_rest = spread(to_imag)
        tables.append(np.concatenate([real_main, imag_main, real_rest, imag_rest], axis=1))
    there = np.stack(tables)
    return as_bf16(there), as_bf16(there.transpose(0, 2, 1))


def half_tables(length):
    half = np.arange(length // 2)
    natural = np.arange(length).reshape(2, length // 16, 8)
    mixed = natural.transpose(1, 0, 2).reshape(-1)
    there, back = [], []
    for parity in (0, 1):
        cosine, sine = phases(np.outer(2 * half + parity, half), length)
        table = np.block([[cosine, -sine], [sine, cosine]])
        there.append(table[:, mixed])
        back.append(table.T)
    return as_bf16(np.stack(there + back))


def column_tables(length, slab):
    cosine, sine = phases(np.outer(np.arange(length), np.arange(length)), length)
    table = np.block([[cosine, -sine], [sine, cosine]])
    order = np.arange(2 * length).reshape(2, length // slab, slab // PLANES, PLANES)
    order = order.transpose(2, 1, 0, 3).reshape(-1)
    there = table[order]
    return as_bf16(there), as_bf16(there.T)


def pick_table(slab):
    lines = PLANES * PAIR
    table = np.zeros((CHUNK, lines * slab))
    for plane in range(PLANES):
        for band in range(PAIR):
            line = plane * PAIR + band
            for part in range(2):
                row = band * 2 * PLANES + part * PLANES + plane
                table[row, line * slab : (line + 1) * slab] = 1.0
    return as_bf16(table)


def whole_kernel(
    mesh_bands,
    orbital_ref,
    slot_ref,
    column_ref,
    previous_ref,
    subspace_hbm,
    pot_ref,
    deep_hbm,
    rise_hbm,
    line_hbm,
    turn_hbm,
    half_hbm,
    pick_ref,
    applied_ref,
    inter_ref,
    subspace_ref,
    deep_ref,
    rise_ref,
    line_ref,
    turn_ref,
    half_ref,
    full_ref,
    left_ref,
    right_ref,
    wave_ref,
    found_ref,
    kinetic_ref,
    hot_ref,
    gather_ref,
    sent_ref,
    stick_ref,
    coord_ref,
    coords_ref,
    mask_ref,
    there_ref,
    again_ref,
    mixed_ref,
    heavy_ref,
    after_ref,
    kept_ref,
    stage_ref,
    back_ref,
    every_ref,
    right_side_ref,
    share_ref,
    shares_ref,
    load_sem,
    recv_sem,
    home_recv,
    once_sem,
):
    slab, size, _ = pot_ref.shape
    owners = size // slab
    half_owners = owners // 2
    half = size // 2
    fold = size // FOLD
    groups_pair = slab // PLANES
    waves = slot_ref.shape[1]
    blocks = waves // LANES
    sticks = LANES
    lines = PLANES * PAIR
    bands = orbital_ref.shape[0]
    pairs = bands // PAIR
    groups = pairs * groups_pair
    rest = size - LANES
    scale = 1.0 / (size * size)
    mine = subspace_ref.shape[0]
    share = share_ref.shape[1]
    shares = mine // share
    me = lax.axis_index("fft")
    band_me = lax.axis_index("band")
    every_band = [lax.rem(band_me + shift, mesh_bands) for shift in range(mesh_bands)]
    others = [lax.rem(me + shift, owners) for shift in range(1, owners)]
    f32, bf16 = jnp.float32, jnp.bfloat16

    def dot(left, right):
        return jnp.dot(left, right, preferred_element_type=f32)

    def halves_dot(table_ref, right):
        return jnp.concatenate([dot(table_ref[:size], right), dot(table_ref[size:], right)], axis=0)

    def remote(src, dst, send, recv, target):
        return pltpu.make_async_remote_copy(
            src_ref=src,
            dst_ref=dst,
            send_sem=send,
            recv_sem=recv,
            device_id=target,
            device_id_type=pl.DeviceIdType.MESH,
        )

    def coord_copy(place):
        return remote(
            coord_ref,
            coords_ref.at[me],
            once_sem.at[0],
            once_sem.at[1],
            {"fft": others[place]},
        )

    def band_copy(place):
        return remote(
            previous_ref,
            every_ref.at[band_me],
            once_sem.at[2],
            once_sem.at[3],
            {"band": every_band[place + 1]},
        )

    def share_copy(block, place):
        return remote(
            share_ref.at[block],
            shares_ref.at[me],
            once_sem.at[4],
            once_sem.at[5],
            {"band": every_band[place], "fft": shares * band_me + block},
        )

    def await_bytes(region, sem):
        pltpu.make_async_copy(region, region, sem).wait()

    def there_copy(group, place):
        return remote(
            sent_ref.at[group, others[place]],
            stick_ref.at[group, me],
            once_sem.at[6],
            recv_sem.at[group],
            {"fft": others[place]},
        )

    def home_copy(group, place):
        return remote(
            stage_ref.at[group + 2, others[place]],
            back_ref.at[group, me],
            once_sem.at[7],
            home_recv.at[group],
            {"fft": others[place]},
        )

    loads = []
    for place, (src, dst) in enumerate(
        (
            (deep_hbm, deep_ref),
            (line_hbm, line_ref),
            (turn_hbm, turn_ref),
            (subspace_hbm, subspace_ref),
            (pot_ref, full_ref),
            (pot_ref.at[:, :, :LANES], left_ref),
            (half_hbm, half_ref),
            (rise_hbm, rise_ref),
        )
    ):
        loads.append(pltpu.make_async_copy(src, dst, load_sem.at[place]))
        loads[-1].start()

    barrier = pltpu.get_barrier_semaphore()
    for place in range(mesh_bands):
        for other in [me] + others:
            if place or other is not me:
                pl.semaphore_signal(
                    barrier,
                    inc=1,
                    device_id={"band": every_band[place], "fft": other},
                    device_id_type=pl.DeviceIdType.MESH,
                )

    low_lane = lax.broadcasted_iota(jnp.int32, (1, LANES), 1) < rest
    level = lax.broadcasted_iota(jnp.int32, (fold, LANES), 0)
    wave_ref[...] = orbital_ref[...].reshape(2 * bands, waves).astype(f32)

    column = column_ref[...]
    grid_x = jnp.floor((column.astype(f32) + 0.5) * (1.0 / size))
    grid_y = column.astype(f32) - grid_x * size
    coord_row = lax.broadcasted_iota(jnp.int32, (8, LANES), 0)
    first_x = lax.convert_element_type(me * slab, f32)
    coord_ref[...] = jnp.where(coord_row == 0, grid_x - first_x, jnp.where(coord_row == 1, grid_y, 0.0))

    def lanes_of(block, count=1):
        return pl.ds(pl.multiple_of(block * LANES, LANES), count * LANES)

    def plane_of(block):
        return lax.shift_right_logical(slot_ref[:, lanes_of(block)], 7)

    @pl.loop(0, blocks, unroll=4)
    def _(block):
        slot = slot_ref[:, lanes_of(block)]
        plane = plane_of(block)
        cell = jnp.bitwise_and(slot, sticks - 1)
        for side in range(1, FOLD):
            cell = cell + jnp.where(plane >= side * fold, sticks, 0)
        rows = lax.broadcasted_iota(jnp.int32, (FOLD * sticks, LANES), 0)
        hot_ref[:, lanes_of(block)] = jnp.where(cell == rows, 1.0, 0.0).astype(bf16)

    pl.semaphore_wait(barrier, mesh_bands * owners - 1)
    for place in range(owners - 1):
        coord_copy(place).start()
    for place in range(mesh_bands - 1):
        band_copy(place).start()
    coords_ref[me] = coord_ref[...]
    every_ref[band_me] = previous_ref[...]

    def level_mask(block):
        plane = plane_of(block)
        for side in range(1, FOLD):
            base = jnp.where(plane >= side * fold, side * fold, 0 if side == 1 else base)
        return plane - base == level

    cells = None
    for block in range(0, blocks, 2):
        pieces = []
        for step in range(2):
            chosen = level_mask(block + step)
            values = wave_ref[:, lanes_of(block + step)]
            rows = [jnp.where(chosen, values[row : row + 1], 0.0) for row in range(2 * bands)]
            pieces.append(jnp.concatenate(rows, axis=0))
        left = jnp.concatenate(pieces, axis=1).astype(bf16)
        term = lax.dot_general(
            left,
            hot_ref[:, lanes_of(block, 2)],
            (((1,), (1,)), ((), ())),
            preferred_element_type=f32,
        )
        cells = term if cells is None else cells + term
    columns = []
    for band in range(bands):
        pieces = []
        for part in range(2):
            start = (2 * band + part) * fold
            for side in range(FOLD):
                pieces.append(cells[start : start + fold, side * LANES : (side + 1) * LANES])
        columns.append(jnp.concatenate(pieces, axis=0))
    columns = jnp.concatenate(columns, axis=1).astype(bf16)
    loads[0].wait()
    along = dot(deep_ref[...], columns).reshape(groups_pair * owners, 2 * PLANES, bands * LANES)
    for pair in range(pairs):
        chunks = []
        for band in range(PAIR * pair, PAIR * (pair + 1)):
            chunks.append(along[:, :, band * LANES : (band + 1) * LANES])
        sent_ref[pair * groups_pair : (pair + 1) * groups_pair] = (
            jnp.concatenate(chunks, axis=1)
            .astype(bf16)
            .reshape(groups_pair, owners, CHUNK, LANES)
        )

    @pl.loop(0, groups)
    def _(group):
        for place in range(owners - 1):
            there_copy(group, place).start()
        stick_ref[group, me] = sent_ref[group, me]

    freq_x = jnp.where(grid_x >= half, grid_x - size, grid_x)
    freq_y = jnp.where(grid_y >= half, grid_y - size, grid_y)
    freq_row = lax.broadcasted_iota(jnp.int32, (16, LANES), 0)
    freqs = jnp.where(freq_row == 0, freq_x, jnp.where(freq_row == 1, freq_y, 0.0))
    freqs = jnp.concatenate([freqs] * FOLD, axis=1).astype(bf16)

    @pl.loop(0, blocks // 8)
    def _(step):
        found = dot(freqs, hot_ref[:, lanes_of(8 * step, 8)])
        plane = lax.shift_right_logical(slot_ref[:, lanes_of(8 * step, 8)], 7)
        freq_z = jnp.where(plane >= half, plane - size, plane).astype(f32)
        total = freq_z * freq_z + found[0:1] * found[0:1] + found[1:2] * found[1:2]
        kinetic_ref[:, lanes_of(8 * step, 8)] = total * (2.0 / (size * size))

    for place in range(1, len(loads)):
        loads[place].wait()

    @pl.loop(0, slab, unroll=4)
    def _(plane):
        local = full_ref[plane, :, LANES:]
        right_ref[plane] = jnp.concatenate([local, local], axis=1)

    await_bytes(coords_ref.at[: owners - 1], once_sem.at[1])

    @pl.loop(0, owners // 2, unroll=2)
    def _(step):
        local = lax.broadcasted_iota(jnp.int32, (slab, sticks), 0).astype(f32)
        cells = lax.broadcasted_iota(jnp.int32, (size, sticks), 0).astype(f32)
        hots = []
        for side in range(2):
            coords = coords_ref[2 * step + side]
            mask_ref[2 * step + side] = jnp.where(coords[0:1, :] == local, 1.0, 0.0)
            hots.append(jnp.where(coords[1:2, :] == cells, 1.0, 0.0))
        hot = jnp.concatenate(hots, axis=1).astype(bf16)
        for part in range(2):
            place = slice(part * sticks, (part + 1) * sticks)
            rows = lax.dot_general(
                hot, line_ref[part], (((0,), (0,)), ((), ())), preferred_element_type=f32
            ).astype(bf16)
            turned = dot(turn_ref[part], hot).astype(bf16)
            for side in range(2):
                mine_here = slice(side * sticks, (side + 1) * sticks)
                there_ref[2 * step + side, place, :] = rows[mine_here]
                again_ref[2 * step + side, :, place] = turned[:, mine_here]

    await_bytes(every_ref.at[: mesh_bands - 1], once_sem.at[3])

    count = mesh_bands * bands
    others_side = every_ref[...].reshape(count, 2, waves).astype(f32)
    right_side_ref[:count] = others_side[:, 0].astype(bf16)
    right_side_ref[count : 2 * count] = others_side[:, 1].astype(bf16)
    own_side = subspace_ref[...].astype(f32)
    own_side = jnp.concatenate([own_side[:, 0], own_side[:, 1]], axis=0).astype(bf16)
    products = lax.dot_general(
        own_side, right_side_ref[...], (((1,), (1,)), ((), ())), preferred_element_type=f32
    )
    lane = lax.broadcasted_iota(jnp.int32, (1, LANES), 1)
    upper, lower = products[:mine], products[mine:]
    blend = jnp.where(
        lane < count,
        upper + pltpu.roll(lower, LANES - count, 1),
        upper - pltpu.roll(lower, count, 1),
    )
    for block in range(shares):
        share_ref[block] = blend[block * share : (block + 1) * share]

    source_band = lax.div(me, shares)
    for block in range(shares):
        for place in range(mesh_bands):
            if place:
                share_copy(block, place).start()
            else:
                to_self = shares * band_me + block == me

                @pl.when(jnp.logical_not(to_self))
                def _():
                    share_copy(block, place).start()

                @pl.when(to_self)
                def _():
                    shares_ref[me] = share_ref[block]

    def spread_lines(group):
        for low in range(half_owners):
            results = []
            for owner in (low, low + half_owners):
                values = stick_ref[group, owner].astype(f32)
                mask = mask_ref[owner]
                parts = []
                for part in range(2):
                    pieces = []
                    for plane in range(PLANES):
                        for band in range(PAIR):
                            row = band * 2 * PLANES + part * PLANES + plane
                            pieces.append(values[row : row + 1, :] * mask)
                    parts.append(jnp.concatenate(pieces, axis=0))
                left = jnp.concatenate(parts, axis=1).astype(bf16)
                results.append(dot(left, there_ref[owner]))
            for plane in range(PLANES):
                unit, side = plane // 2, plane % 2
                start = plane * PAIR * slab

                def pieces_of(result):
                    one = result[start : start + slab]
                    two = result[start + slab : start + 2 * slab]
                    found = []
                    for half_lines in (one, two):
                        found.append((half_lines[:, :LANES], half_lines[:, LANES : 2 * LANES]))
                    both = []
                    for offset in (2 * LANES, 3 * LANES):
                        both.append(
                            jnp.where(
                                low_lane,
                                one[:, offset : offset + LANES],
                                two[:, offset : offset + LANES],
                            )
                        )
                    found.append(tuple(both))
                    return found

                near, far = pieces_of(results[0]), pieces_of(results[1])
                offsets = (2 * side * LANES, (2 * side + 1) * LANES, (4 + side) * LANES)
                for (near_re, near_im), (far_re, far_im), offset in zip(near, far, offsets):
                    for parity in range(2):
                        if parity == 0:
                            real, imag = near_re + far_re, near_im + far_im
                        else:
                            real, imag = near_re - far_re, near_im - far_im
                        tile = jnp.concatenate(
                            [real.reshape(-1, 8, LANES), imag.reshape(-1, 8, LANES)], axis=1
                        )
                        mixed_ref[
                            unit,
                            parity,
                            slice(2 * slab * low, 2 * slab * (low + 1)),
                            offset : offset + LANES,
                        ] = tile.reshape(2 * slab, LANES).astype(bf16)

    def forward_lines(group, unit):
        first = lax.rem(group, groups_pair) * PLANES
        if True:
            for parity in range(2):
                picks = pl.ds(parity, half, 2)

                for tile in range(3):
                    result = dot(
                        half_ref[parity],
                        mixed_ref[unit, parity, :, 2 * LANES * tile : 2 * LANES * (tile + 1)],
                    )
                    if tile < 2:
                        local = left_ref[first + 2 * unit + tile, picks, :]
                        local = jnp.concatenate([local, local], axis=1)
                    else:
                        one = right_ref[first + 2 * unit, picks, :]
                        two = right_ref[first + 2 * unit + 1, picks, :]
                        local = jnp.concatenate([one, two], axis=1)
                    heavy_ref[unit, parity, tile, :half] = (result[:half] * local).astype(bf16)
                    heavy_ref[unit, parity, tile, half:] = (result[half:] * local).astype(bf16)

    def backward_lines(unit):
        if True:
            for tile in range(3):
                even = dot(half_ref[2], heavy_ref[unit, 0, tile])
                odd = dot(half_ref[3], heavy_ref[unit, 1, tile])
                for side, values in enumerate((even + odd, even - odd)):
                    for low in range(half_owners):
                        owner = low + side * half_owners
                        for part in range(2):
                            start = part * half + low * slab
                            found = values[start : start + slab]
                            one, two = found[:, :LANES], found[:, LANES:]
                            if tile < 2:
                                rows = pl.ds(
                                    pl.multiple_of((2 * unit + tile) * 2 * slab, 2 * slab), 2 * slab
                                )
                                after_ref[owner, rows, part * LANES : (part + 1) * LANES] = (
                                    jnp.concatenate([one, two], axis=0).astype(bf16)
                                )
                            else:
                                for place, both in enumerate((one, two)):
                                    plane = 2 * unit + place
                                    rows = pl.ds(
                                        pl.multiple_of(plane * 2 * slab, 2 * slab), 2 * slab
                                    )
                                    after_ref[
                                        owner, rows, (2 + part) * LANES : (3 + part) * LANES
                                    ] = jnp.concatenate(
                                        [
                                            jnp.where(low_lane, both, 0.0),
                                            jnp.where(low_lane, 0.0, both),
                                        ],
                                        axis=0,
                                    ).astype(bf16)

    part_row = lax.broadcasted_iota(jnp.int32, (CHUNK, LANES), 0)
    part_row = jnp.bitwise_and(part_row, PLANES) == 0

    def weighed_lines():
        for owner in range(owners):
            result = dot(after_ref[owner], again_ref[owner])
            mask = mask_ref[owner] * scale
            mask = jnp.concatenate([mask, mask], axis=1)[None]
            kept = (result.reshape(lines, slab, 2 * LANES) * mask).reshape(lines * slab, 2 * LANES)
            kept_ref[owner] = kept.astype(bf16)

    def picked_lines(place):
        for owner in range(owners):
            found = dot(pick_ref[...], kept_ref[owner])
            stage_ref[place, owner] = jnp.where(
                part_row, found[:, :LANES], found[:, LANES:]
            ).astype(bf16)

    def wait_group(group):
        await_bytes(stick_ref.at[group, : owners - 1], recv_sem.at[group])

    def send_home(group):
        for place in range(owners - 1):
            home_copy(group, place).start()
        back_ref[group, me] = stage_ref[group + 2, me]

    wait_group(0)
    spread_lines(0)

    @pl.loop(0, groups)
    def _(group):
        @pl.when(group < groups - 1)
        def _():
            wait_group(group + 1)

        forward_lines(group, 0)
        forward_lines(group, 1)
        picked_lines(group)
        weighed_lines()
        backward_lines(0)
        backward_lines(1)
        spread_lines(lax.rem(group + 1, groups))

        @pl.when(group > 1)
        def _():
            send_home(group - 2)

    picked_lines(groups)
    weighed_lines()
    send_home(groups - 2)
    picked_lines(groups + 1)
    send_home(groups - 1)

    def gather_waves(pair):
        first = pair * groups_pair

        @pl.loop(0, groups_pair)
        def _(step):
            await_bytes(back_ref.at[first + step, : owners - 1], home_recv.at[first + step])

        chunks = back_ref[first : first + groups_pair].reshape(groups_pair * owners, CHUNK, LANES)
        chunks = chunks.astype(f32)
        columns = []
        for band in range(PAIR):
            rows = chunks[:, band * 2 * PLANES : (band + 1) * 2 * PLANES]
            columns.append(rows.reshape(2 * size, LANES))
        columns = jnp.concatenate(columns, axis=1).astype(bf16)
        risen = (halves_dot(rise_ref, columns) * (1.0 / size)).astype(bf16)
        pieces = []
        for band in range(PAIR):
            for part in range(2):
                sides = []
                for side in range(FOLD):
                    start = part * size + side * fold
                    sides.append(risen[start : start + fold, band * LANES : (band + 1) * LANES])
                pieces.append(jnp.concatenate(sides, axis=1))
        gather_ref[...] = jnp.concatenate(pieces, axis=0)

        @pl.loop(0, blocks // 2, unroll=4)
        def _(step):
            values = dot(gather_ref[...], hot_ref[:, lanes_of(2 * step, 2)])
            for side in range(2):
                chosen = level_mask(2 * step + side)
                for part in range(2 * PAIR):
                    ours = values[part * fold : (part + 1) * fold, side * LANES : (side + 1) * LANES]
                    row = 2 * PAIR * pair + part
                    found_ref[row : row + 1, lanes_of(2 * step + side)] = jnp.sum(
                        jnp.where(chosen, ours, 0.0), axis=0, keepdims=True
                    )

    for pair in range(pairs):
        gather_waves(pair)

    result = found_ref[...] + kinetic_ref[...] * wave_ref[...]
    applied_ref[...] = result.astype(bf16).reshape(bands, 2, waves)

    inside = source_band == band_me

    @pl.when(inside)
    def _():
        await_bytes(shares_ref.at[: mesh_bands * shares - 1], once_sem.at[4])
        await_bytes(shares_ref.at[: owners - 1], once_sem.at[5])

    @pl.when(jnp.logical_not(inside))
    def _():
        await_bytes(shares_ref.at[: mesh_bands * shares], once_sem.at[4])
        await_bytes(shares_ref, once_sem.at[5])

    await_bytes(coords_ref.at[: owners - 1], once_sem.at[0])
    await_bytes(every_ref.at[: mesh_bands - 1], once_sem.at[2])
    await_bytes(stick_ref.at[:, : owners - 1], once_sem.at[6])
    await_bytes(back_ref.at[:, : owners - 1], once_sem.at[7])

    total = shares_ref[0]
    for source in range(1, owners):
        total = total + shares_ref[source]
    total = pltpu.roll(total, lax.rem(LANES - bands * band_me, LANES), 1)
    inter_ref[...] = total


def whole_work(mesh_bands, orbitals, slots, columns, potential, subspace, previous):
    slab, size, _ = potential.shape
    owners = size // slab
    groups_pair = slab // PLANES
    bands, _, waves = orbitals.shape
    groups = bands // PAIR * groups_pair
    half = size // 2
    lines = PLANES * PAIR
    mine = subspace.shape[0]
    share = mine * mesh_bands // owners
    deep, rise = column_tables(size, slab)
    line, turn = line_tables(size)
    halves = half_tables(size)
    pick = pick_table(slab)
    in_vmem = pl.BlockSpec(memory_space=pltpu.VMEM)
    anywhere = pl.BlockSpec(memory_space=pl.ANY)
    bf16, f32 = jnp.bfloat16, jnp.float32
    dma = pltpu.SemaphoreType.DMA
    return pl.pallas_call(
        functools.partial(whole_kernel, mesh_bands),
        out_shape=(
            jax.ShapeDtypeStruct(orbitals.shape, bf16),
            jax.ShapeDtypeStruct((share, LANES), f32),
        ),
        in_specs=[in_vmem] * 4 + [anywhere] * 7 + [in_vmem],
        out_specs=(in_vmem, in_vmem),
        scratch_shapes=[
            pltpu.VMEM(subspace.shape, bf16),
            pltpu.VMEM(deep.shape, bf16),
            pltpu.VMEM(rise.shape, bf16),
            pltpu.VMEM(line.shape, bf16),
            pltpu.VMEM(turn.shape, bf16),
            pltpu.VMEM(halves.shape, bf16),
            pltpu.VMEM((slab, size, size), f32),
            pltpu.VMEM((slab, size, LANES), f32),
            pltpu.VMEM((slab, size, LANES), f32),
            pltpu.VMEM((2 * bands, waves), f32),
            pltpu.VMEM((2 * bands, waves), f32),
            pltpu.VMEM((1, waves), f32),
            pltpu.VMEM((FOLD * LANES, waves), bf16),
            pltpu.VMEM((2 * PAIR * size // FOLD, FOLD * LANES), bf16),
            pltpu.VMEM((groups, owners, CHUNK, LANES), bf16),
            pltpu.VMEM((groups, owners, CHUNK, LANES), bf16),
            pltpu.VMEM((8, LANES), f32),
            pltpu.VMEM((owners, 8, LANES), f32),
            pltpu.VMEM((owners, slab, LANES), f32),
            pltpu.VMEM((owners, 2 * LANES, 4 * LANES), bf16),
            pltpu.VMEM((owners, 4 * LANES, 2 * LANES), bf16),
            pltpu.VMEM((PLANES // 2, 2, size, 6 * LANES), bf16),
            pltpu.VMEM((PLANES // 2, 2, 3, size, 2 * LANES), bf16),
            pltpu.VMEM((owners, lines * slab, 4 * LANES), bf16),
            pltpu.VMEM((owners, lines * slab, 2 * LANES), bf16),
            pltpu.VMEM((groups + 2, owners, CHUNK, LANES), bf16),
            pltpu.VMEM((groups, owners, CHUNK, LANES), bf16),
            pltpu.VMEM((mesh_bands, bands, 2, waves), bf16),
            pltpu.VMEM((LANES, waves), bf16),
            pltpu.VMEM((mine // share, share, LANES), f32),
            pltpu.VMEM((owners, share, LANES), f32),
            dma((8,)),
            dma((groups,)),
            dma((groups,)),
            dma((8,)),
        ],
        compiler_params=pltpu.CompilerParams(
            collective_id=0, has_side_effects=True, vmem_limit_bytes=60 * 1024 * 1024
        ),
        cost_estimate=pl.CostEstimate(
            flops=40 * 10**9, bytes_accessed=8 * 10**6, transcendentals=0
        ),
    )(
        orbitals,
        slots,
        columns,
        previous,
        subspace,
        potential,
        deep,
        rise,
        line,
        turn,
        halves,
        pick,
    )


def hand_out(bands, count, applied_in, total_in, applied_ref, inter_ref):
    applied_ref[...] = applied_in[...]
    total = total_in[...].T
    inter_ref[0] = total[:bands]
    inter_ref[1] = total[count : count + bands]


def handed_out(mesh_bands, applied, total):
    bands, share = applied.shape[0], total.shape[0]
    in_vmem = pl.BlockSpec(memory_space=pltpu.VMEM)
    return pl.pallas_call(
        functools.partial(hand_out, bands, mesh_bands * bands),
        out_shape=(
            jax.ShapeDtypeStruct(applied.shape, jnp.bfloat16),
            jax.ShapeDtypeStruct((2, bands, share), jnp.float32),
        ),
        in_specs=[in_vmem] * 2,
        out_specs=(in_vmem, in_vmem),
    )(applied, total)


def fast_device(mesh_bands, orbitals, sphere_slot, stick_column, potential, subspace, previous):
    slots = sphere_slot.reshape(1, -1)
    columns = stick_column.reshape(1, -1)
    arrays = (orbitals, slots, columns, potential, subspace, previous)
    applied, total = whole_work(mesh_bands, *arrays)
    applied, turned = handed_out(mesh_bands, applied, total)
    return applied, turned.transpose(0, 2, 1)


def fits(mesh_bands, orbitals, slots, sticks, potential, subspace, previous):
    slab, size, _ = potential.shape
    owners = size // slab
    bands, mine = orbitals.shape[0], subspace.shape[0]
    good = slab % 8 == 0 and owners % 2 == 0 and owners * slab == size
    good = good and 2 * size == 3 * LANES and sticks.shape[0] == LANES
    good = good and bands % PAIR == 0 and slots.shape[0] % (8 * LANES) == 0
    good = good and mine * mesh_bands % (8 * owners) == 0 and owners % mesh_bands == 0
    return good and 2 * mesh_bands * bands <= LANES


def per_device(mesh_bands, *arrays):
    if fits(mesh_bands, *arrays):
        return fast_device(mesh_bands, *arrays)
    return general_device(*arrays)


def solution(mesh):
    return jax.shard_map(
        functools.partial(per_device, mesh.shape["band"]),
        mesh=mesh,
        in_specs=(
            P("band", None, "fft"),
            P("fft"),
            P("fft"),
            P("fft", None, None),
            P("band", None, "fft"),
            P("band", None, "fft"),
        ),
        out_specs=(P("band", None, "fft"), P(None, "fft", "band")),
        check_vma=False,
    )
```

```python
import functools
import math

import jax
import jax.numpy as jnp
import numpy as np
from jax import lax
from jax.experimental import pallas as pl
from jax.experimental.pallas import tpu as pltpu
from jax.sharding import PartitionSpec as P


def dft_table(length, sign_value, factor):
    positions = jnp.arange(length, dtype=jnp.int32)
    phase_step = positions[:, None] * positions[None, :] % length
    angle_value = phase_step.astype(jnp.float32) * (2.0 * math.pi / length)
    cosine = (jnp.cos(angle_value) * factor).astype(jnp.bfloat16)
    sine_part = (jnp.sin(angle_value) * (sign_value * factor)).astype(jnp.bfloat16)
    return (cosine, sine_part)


def apply_dft(real_in, imag_in, table, form):
    cosine, sine_part = table

    def product(operand, table_part):
        return jnp.einsum(form, operand, table_part, preferred_element_type=jnp.float32)

    real_out = product(real_in, cosine) - product(imag_in, sine_part)
    imag_out = product(real_in, sine_part) + product(imag_in, cosine)
    return (real_out, imag_out)


def packed(pair, axis_pos):
    return jnp.stack([pair[0].astype(jnp.bfloat16), pair[1].astype(jnp.bfloat16)], axis=axis_pos)


def frequency(values, grid_size):
    return jnp.where(values >= grid_size // 2, values - grid_size, values).astype(jnp.float32)


def one_hot_rows(indices, count):
    return (indices[None, :] == jnp.arange(count, dtype=jnp.int32)[:, None]).astype(jnp.bfloat16)


def general_device(orbitals, sphere_slot, stick_column, potential, subspace, previous):
    slab_depth = potential.shape[0]
    grid_size = potential.shape[1]
    stick_count = stick_column.shape[0]
    slab_cells = slab_depth * grid_size
    forward = dft_table(grid_size, 1.0, 1.0)
    inverse = dft_table(grid_size, -1.0, 1.0 / grid_size)
    plane_index = sphere_slot // stick_count
    stick_index = sphere_slot % stick_count
    plane_hot = one_hot_rows(plane_index, grid_size)
    stick_hot = one_hot_rows(stick_index, stick_count)
    stick_coords = jnp.stack([stick_column // grid_size, stick_column % grid_size]).astype(
        jnp.bfloat16
    )
    wave_coords = jnp.dot(stick_coords, stick_hot, preferred_element_type=jnp.float32)
    freq_z = frequency(plane_index, grid_size)
    freq_x = frequency(wave_coords[0].astype(jnp.int32), grid_size)
    freq_y = frequency(wave_coords[1].astype(jnp.int32), grid_size)
    kinetic = (freq_z * freq_z + freq_x * freq_x + freq_y * freq_y) * (
        2.0 / (grid_size * grid_size)
    )
    prev_real = previous[:, 0]
    prev_imag = previous[:, 1]
    sub_piece = lax.all_gather(subspace, "band", axis=0, tiled=True)
    sub_real = sub_piece[:, 0]
    sub_imag = sub_piece[:, 1]
    over_real = jnp.einsum(
        "jg,ig->ji", sub_real, prev_real, preferred_element_type=jnp.float32
    ) + jnp.einsum("jg,ig->ji", sub_imag, prev_imag, preferred_element_type=jnp.float32)
    over_imag = jnp.einsum(
        "jg,ig->ji", sub_real, prev_imag, preferred_element_type=jnp.float32
    ) - jnp.einsum("jg,ig->ji", sub_imag, prev_real, preferred_element_type=jnp.float32)
    partial_value = jnp.stack([over_real, over_imag])
    intersection = lax.psum_scatter(partial_value, "fft", scatter_dimension=1, tiled=True)
    stick_buffer = jnp.einsum(
        "bpi,zi,si->bpzs", orbitals, plane_hot, stick_hot, preferred_element_type=jnp.float32
    ).astype(jnp.bfloat16)

    def potential_work(along_y):
        along_x = apply_dft(along_y[0], along_y[1], forward, "zxy,xk->zky")
        weighted = packed((along_x[0] * potential, along_x[1] * potential), 0)
        back_x = packed(apply_dft(weighted[0], weighted[1], inverse, "zxy,xk->zky"), 0)
        return packed(apply_dft(back_x[0], back_x[1], inverse, "zxy,yk->zxk"), 0)

    along_z = packed(apply_dft(stick_buffer[:, 0], stick_buffer[:, 1], forward, "bzs,zk->bks"), 1)
    all_columns = lax.all_gather(stick_column, "fft", axis=0, tiled=True)
    owners = all_columns.shape[0] // stick_count
    block_columns = (all_columns % slab_cells).reshape(owners, stick_count)
    block_hot = (
        block_columns[:, :, None] == jnp.arange(slab_cells, dtype=jnp.int32)[None, None, :]
    ).astype(jnp.bfloat16)

    def stick_work(one_band):
        plane_depth = one_band.shape[1]
        split_band = one_band.reshape(2, plane_depth, owners, stick_count)
        plane_grid = jnp.einsum(
            "pzds,dsc->pzdc", split_band, block_hot, preferred_element_type=jnp.float32
        ).astype(jnp.bfloat16)
        plane_grid = plane_grid.reshape(2, plane_depth, grid_size, grid_size)
        along_y = packed(apply_dft(plane_grid[0], plane_grid[1], forward, "zxy,yk->zxk"), 0)
        back_y = potential_work(along_y)
        back_split = back_y.reshape(2, plane_depth, owners, slab_cells)
        picked = jnp.einsum(
            "pzdc,dsc->pzds", back_split, block_hot, preferred_element_type=jnp.float32
        ).astype(jnp.bfloat16)
        return picked.reshape(2, plane_depth, owners * stick_count)

    finished = lax.map(
        stick_work, lax.all_to_all(along_z, "fft", split_axis=2, concat_axis=3, tiled=True)
    )
    stick_values = lax.all_to_all(finished, "fft", split_axis=3, concat_axis=2, tiled=True)
    picked_sticks = jnp.einsum(
        "bpzs,si->bpzi", stick_values, stick_hot, preferred_element_type=jnp.float32
    ).astype(jnp.bfloat16)
    cosine_cols = jnp.einsum("zk,ki->zi", inverse[0], plane_hot, preferred_element_type=jnp.float32)
    sine_cols = jnp.einsum("zk,ki->zi", inverse[1], plane_hot, preferred_element_type=jnp.float32)
    pick_real = picked_sticks[:, 0].astype(jnp.float32)
    pick_imag = picked_sticks[:, 1].astype(jnp.float32)
    wave_real = jnp.sum(pick_real * cosine_cols[None] - pick_imag * sine_cols[None], axis=1)
    wave_imag = jnp.sum(pick_real * sine_cols[None] + pick_imag * cosine_cols[None], axis=1)
    real_out = wave_real + kinetic * orbitals[:, 0].astype(jnp.float32)
    imag_out = wave_imag + kinetic * orbitals[:, 1].astype(jnp.float32)
    applied = jnp.stack([real_out, imag_out], axis=1).astype(jnp.bfloat16)
    return (applied, intersection)


PLANES = 4
PAIR = 2
LANES = 128
CHUNK = 4 * PLANES
FOLD = 4


def phases(products, length):
    angle = (products % length).astype(np.float64) * (2.0 * np.pi / length)
    return np.cos(angle), np.sin(angle)


def as_bf16(array):
    return jnp.asarray(array, jnp.bfloat16)


def line_tables(length):
    cosine, sine = phases(np.outer(np.arange(length), np.arange(length)), length)

    def spread(table):
        rest = table[:, LANES:]
        return table[:, :LANES], np.concatenate([rest, rest], axis=1)

    tables = []
    for to_real, to_imag in ((cosine, sine), (-sine, cosine)):
        real_main, real_rest = spread(to_real)
        imag_main, imag_rest = spread(to_imag)
        tables.append(np.concatenate([real_main, imag_main, real_rest, imag_rest], axis=1))
    there = np.stack(tables)
    return as_bf16(there), as_bf16(there.transpose(0, 2, 1))


def half_tables(length):
    half = np.arange(length // 2)
    natural = np.arange(length).reshape(2, length // 16, 8)
    mixed = natural.transpose(1, 0, 2).reshape(-1)
    there, back = [], []
    for parity in (0, 1):
        cosine, sine = phases(np.outer(2 * half + parity, half), length)
        table = np.block([[cosine, -sine], [sine, cosine]])
        there.append(table[:, mixed])
        back.append(table.T)
    return as_bf16(np.stack(there + back))


def column_tables(length, slab):
    cosine, sine = phases(np.outer(np.arange(length), np.arange(length)), length)
    table = np.block([[cosine, -sine], [sine, cosine]])
    order = np.arange(2 * length).reshape(2, length // slab, slab // PLANES, PLANES)
    order = order.transpose(2, 1, 0, 3).reshape(-1)
    there = table[order]
    return as_bf16(there), as_bf16(there.T)


def pick_table(slab):
    lines = PLANES * PAIR
    table = np.zeros((CHUNK, lines * slab))
    for plane in range(PLANES):
        for band in range(PAIR):
            line = plane * PAIR + band
            for part in range(2):
                row = band * 2 * PLANES + part * PLANES + plane
                table[row, line * slab : (line + 1) * slab] = 1.0
    return as_bf16(table)


def whole_kernel(
    mesh_bands,
    orbital_hbm,
    slot_hbm,
    column_hbm,
    previous_hbm,
    subspace_hbm,
    pot_ref,
    deep_hbm,
    rise_hbm,
    line_hbm,
    turn_hbm,
    half_hbm,
    pick_hbm,
    applied_ref,
    inter_ref,
    orbital_ref,
    slot_ref,
    column_ref,
    previous_ref,
    pick_ref,
    subspace_ref,
    deep_ref,
    rise_ref,
    line_ref,
    turn_ref,
    half_ref,
    full_ref,
    left_ref,
    right_ref,
    wave_ref,
    found_ref,
    kinetic_ref,
    hot_ref,
    gather_ref,
    sent_ref,
    stick_ref,
    coord_ref,
    coords_ref,
    mask_ref,
    there_ref,
    again_ref,
    mixed_ref,
    heavy_ref,
    after_ref,
    kept_ref,
    stage_ref,
    back_ref,
    every_ref,
    right_side_ref,
    blend_ref,
    share_ref,
    shares_ref,
    load_sem,
    recv_sem,
    home_recv,
    once_sem,
):
    slab, size, _ = pot_ref.shape
    owners = size // slab
    half_owners = owners // 2
    half = size // 2
    fold = size // FOLD
    groups_pair = slab // PLANES
    waves = slot_ref.shape[1]
    blocks = waves // LANES
    sticks = LANES
    lines = PLANES * PAIR
    bands = orbital_ref.shape[0]
    pairs = bands // PAIR
    groups = pairs * groups_pair
    rest = size - LANES
    scale = 1.0 / (size * size)
    mine = subspace_ref.shape[0]
    share = share_ref.shape[1]
    shares = mine // share
    me = lax.axis_index("fft")
    band_me = lax.axis_index("band")
    every_band = [lax.rem(band_me + shift, mesh_bands) for shift in range(mesh_bands)]
    others = [lax.rem(me + shift, owners) for shift in range(1, owners)]
    f32, bf16 = jnp.float32, jnp.bfloat16

    def dot(left, right):
        return jnp.dot(left, right, preferred_element_type=f32)

    def halves_dot(table_ref, right):
        return jnp.concatenate([dot(table_ref[:size], right), dot(table_ref[size:], right)], axis=0)

    def remote(src, dst, send, recv, target):
        return pltpu.make_async_remote_copy(
            src_ref=src,
            dst_ref=dst,
            send_sem=send,
            recv_sem=recv,
            device_id=target,
            device_id_type=pl.DeviceIdType.MESH,
        )

    def coord_copy(place):
        return remote(
            coord_ref,
            coords_ref.at[me],
            once_sem.at[0],
            once_sem.at[1],
            {"fft": others[place]},
        )

    def band_copy(place):
        return remote(
            previous_ref,
            every_ref.at[band_me],
            once_sem.at[2],
            once_sem.at[3],
            {"band": every_band[place + 1]},
        )

    def share_copy(block, place):
        return remote(
            share_ref.at[block],
            shares_ref.at[me],
            once_sem.at[4],
            once_sem.at[5],
            {"band": every_band[place], "fft": shares * band_me + block},
        )

    def await_bytes(region, sem):
        pltpu.make_async_copy(region, region, sem).wait()

    bounds = (0, 2, groups_pair, groups)

    def there_copy(batch, place):
        some = slice(bounds[batch], bounds[batch + 1])
        return remote(
            sent_ref.at[some, others[place]],
            stick_ref.at[some, me],
            once_sem.at[6],
            recv_sem.at[batch],
            {"fft": others[place]},
        )

    def home_copy(group, place):
        return remote(
            stage_ref.at[group + 2, others[place]],
            back_ref.at[group, me],
            once_sem.at[7],
            home_recv.at[group],
            {"fft": others[place]},
        )

    barrier = pltpu.get_barrier_semaphore()
    for place in range(mesh_bands):
        for other in [me] + others:
            if place or other is not me:
                pl.semaphore_signal(
                    barrier,
                    inc=1,
                    device_id={"band": every_band[place], "fft": other},
                    device_id_type=pl.DeviceIdType.MESH,
                )

    loads = []
    for place, (src, dst) in enumerate(
        (
            (slot_hbm, slot_ref),
            (orbital_hbm, orbital_ref),
            (column_hbm, column_ref),
            (previous_hbm, previous_ref),
            (deep_hbm, deep_ref),
            (line_hbm, line_ref),
            (turn_hbm, turn_ref),
            (subspace_hbm, subspace_ref),
            (pot_ref, full_ref),
            (pot_ref.at[:, :, :LANES], left_ref),
            (half_hbm, half_ref),
            (pick_hbm, pick_ref),
            (rise_hbm, rise_ref),
        )
    ):
        loads.append(pltpu.make_async_copy(src, dst, load_sem.at[place]))
        loads[-1].start()
    for place in range(4):
        loads[place].wait()

    low_lane = lax.broadcasted_iota(jnp.int32, (1, LANES), 1) < rest
    level = lax.broadcasted_iota(jnp.int32, (fold, LANES), 0)
    wave_ref[...] = orbital_ref[...].reshape(2 * bands, waves).astype(f32)

    column = column_ref[...]
    grid_x = jnp.floor((column.astype(f32) + 0.5) * (1.0 / size))
    grid_y = column.astype(f32) - grid_x * size
    coord_row = lax.broadcasted_iota(jnp.int32, (8, LANES), 0)
    first_x = lax.convert_element_type(me * slab, f32)
    coord_ref[...] = jnp.where(coord_row == 0, grid_x - first_x, jnp.where(coord_row == 1, grid_y, 0.0))

    def lanes_of(block, count=1):
        return pl.ds(pl.multiple_of(block * LANES, LANES), count * LANES)

    def plane_of(block):
        return lax.shift_right_logical(slot_ref[:, lanes_of(block)], 7)

    def hot_of(block):
        stick = jnp.bitwise_and(slot_ref[:, lanes_of(block)], sticks - 1)
        plane = plane_of(block)
        rows = lax.broadcasted_iota(jnp.int32, (sticks, LANES), 0)
        chosen = jnp.where(stick == rows, 1.0, 0.0).astype(bf16).reshape(-1, 16, LANES)
        sides = []
        for side in range(FOLD):
            inside = jnp.logical_and(plane >= side * fold, plane < (side + 1) * fold)
            inside = jnp.broadcast_to(jnp.where(inside, 1.0, 0.0), (16, LANES)).astype(bf16)
            sides.append((chosen * inside[None]).reshape(sticks, LANES))
        return jnp.concatenate(sides, axis=0)

    pl.semaphore_wait(barrier, mesh_bands * owners - 1)
    for place in range(owners - 1):
        coord_copy(place).start()
    for place in range(mesh_bands - 1):
        band_copy(place).start()
    coords_ref[me] = coord_ref[...]
    every_ref[band_me] = previous_ref[...]

    def level_mask(block):
        plane = plane_of(block)
        for side in range(1, FOLD):
            base = jnp.where(plane >= side * fold, side * fold, 0 if side == 1 else base)
        return plane - base == level

    cells = None
    for block in range(0, blocks, 2):
        pieces = []
        hot = jnp.concatenate([hot_of(block), hot_of(block + 1)], axis=1)
        hot_ref[:, lanes_of(block, 2)] = hot
        for step in range(2):
            chosen = level_mask(block + step)
            values = wave_ref[:, lanes_of(block + step)]
            rows = [jnp.where(chosen, values[row : row + 1], 0.0) for row in range(2 * bands)]
            pieces.append(jnp.concatenate(rows, axis=0))
        left = jnp.concatenate(pieces, axis=1).astype(bf16)
        term = lax.dot_general(
            left,
            hot,
            (((1,), (1,)), ((), ())),
            preferred_element_type=f32,
        )
        cells = term if cells is None else cells + term
    columns = []
    for band in range(bands):
        pieces = []
        for part in range(2):
            start = (2 * band + part) * fold
            for side in range(FOLD):
                pieces.append(cells[start : start + fold, side * LANES : (side + 1) * LANES])
        columns.append(jnp.concatenate(pieces, axis=0))
    columns = jnp.concatenate(columns, axis=1).astype(bf16)
    loads[4].wait()
    along = dot(deep_ref[...], columns).reshape(groups_pair * owners, 2 * PLANES, bands * LANES)
    for pair in range(pairs):
        chunks = []
        for band in range(PAIR * pair, PAIR * (pair + 1)):
            chunks.append(along[:, :, band * LANES : (band + 1) * LANES])
        sent_ref[pair * groups_pair : (pair + 1) * groups_pair] = (
            jnp.concatenate(chunks, axis=1)
            .astype(bf16)
            .reshape(groups_pair, owners, CHUNK, LANES)
        )

    for batch in range(2):
        for place in range(owners - 1):
            there_copy(batch, place).start()
    stick_ref[:, me] = sent_ref[:, me]

    for place in range(5, len(loads)):
        loads[place].wait()

    @pl.loop(0, slab, unroll=4)
    def _(plane):
        local = full_ref[plane, :, LANES:]
        right_ref[plane] = jnp.concatenate([local, local], axis=1)

    await_bytes(coords_ref.at[: owners - 1], once_sem.at[1])

    @pl.loop(0, owners // 2, unroll=2)
    def _(step):
        local = lax.broadcasted_iota(jnp.int32, (slab, sticks), 0).astype(f32)
        cells = lax.broadcasted_iota(jnp.int32, (size, sticks), 0).astype(f32)
        hots = []
        for side in range(2):
            coords = coords_ref[2 * step + side]
            mask_ref[2 * step + side] = jnp.where(coords[0:1, :] == local, 1.0, 0.0)
            hots.append(jnp.where(coords[1:2, :] == cells, 1.0, 0.0))
        hot = jnp.concatenate(hots, axis=1).astype(bf16)
        for part in range(2):
            place = slice(part * sticks, (part + 1) * sticks)
            rows = lax.dot_general(
                hot, line_ref[part], (((0,), (0,)), ((), ())), preferred_element_type=f32
            ).astype(bf16)
            turned = dot(turn_ref[part], hot).astype(bf16)
            for side in range(2):
                mine_here = slice(side * sticks, (side + 1) * sticks)
                there_ref[2 * step + side, place, :] = rows[mine_here]
                again_ref[2 * step + side, :, place] = turned[:, mine_here]

    await_bytes(every_ref.at[: mesh_bands - 1], once_sem.at[3])

    count = mesh_bands * bands
    right_side_ref[: 2 * count] = every_ref[...].reshape(2 * count, waves)
    products = lax.dot_general(
        subspace_ref[...].reshape(2 * mine, waves),
        right_side_ref[...],
        (((1,), (1,)), ((), ())),
        preferred_element_type=f32,
    )
    below = pltpu.roll(products, 2 * mine - 1, 0)
    even_lane = jnp.bitwise_and(lax.broadcasted_iota(jnp.int32, (1, LANES), 1), 1) == 0
    blend_ref[...] = jnp.where(
        even_lane,
        products + pltpu.roll(below, LANES - 1, 1),
        products - pltpu.roll(below, 1, 1),
    )
    for block in range(shares):
        share_ref[block] = blend_ref[pl.ds(2 * share * block, share, 2), :]

    source_band = lax.div(me, shares)
    for block in range(shares):
        for place in range(mesh_bands):
            if place:
                share_copy(block, place).start()
            else:
                to_self = shares * band_me + block == me

                @pl.when(jnp.logical_not(to_self))
                def _():
                    share_copy(block, place).start()

                @pl.when(to_self)
                def _():
                    shares_ref[me] = share_ref[block]

    def spread_lines(group):
        for low in range(half_owners):
            results = []
            for owner in (low, low + half_owners):
                values = stick_ref[group, owner].astype(f32)
                mask = mask_ref[owner]
                parts = []
                for part in range(2):
                    pieces = []
                    for plane in range(PLANES):
                        for band in range(PAIR):
                            row = band * 2 * PLANES + part * PLANES + plane
                            pieces.append(values[row : row + 1, :] * mask)
                    parts.append(jnp.concatenate(pieces, axis=0))
                left = jnp.concatenate(parts, axis=1).astype(bf16)
                results.append(dot(left, there_ref[owner]))
            for plane in range(PLANES):
                unit, side = plane // 2, plane % 2
                start = plane * PAIR * slab

                def pieces_of(result):
                    one = result[start : start + slab]
                    two = result[start + slab : start + 2 * slab]
                    found = []
                    for half_lines in (one, two):
                        found.append((half_lines[:, :LANES], half_lines[:, LANES : 2 * LANES]))
                    both = []
                    for offset in (2 * LANES, 3 * LANES):
                        both.append(
                            jnp.where(
                                low_lane,
                                one[:, offset : offset + LANES],
                                two[:, offset : offset + LANES],
                            )
                        )
                    found.append(tuple(both))
                    return found

                near, far = pieces_of(results[0]), pieces_of(results[1])
                offsets = (2 * side * LANES, (2 * side + 1) * LANES, (4 + side) * LANES)
                for (near_re, near_im), (far_re, far_im), offset in zip(near, far, offsets):
                    for parity in range(2):
                        if parity == 0:
                            real, imag = near_re + far_re, near_im + far_im
                        else:
                            real, imag = near_re - far_re, near_im - far_im
                        tile = jnp.concatenate(
                            [real.reshape(-1, 8, LANES), imag.reshape(-1, 8, LANES)], axis=1
                        )
                        mixed_ref[
                            unit,
                            parity,
                            slice(2 * slab * low, 2 * slab * (low + 1)),
                            offset : offset + LANES,
                        ] = tile.reshape(2 * slab, LANES).astype(bf16)

    def forward_lines(group, unit):
        first = lax.rem(group, groups_pair) * PLANES
        if True:
            for parity in range(2):
                picks = pl.ds(parity, half, 2)

                for tile in range(3):
                    result = dot(
                        half_ref[parity],
                        mixed_ref[unit, parity, :, 2 * LANES * tile : 2 * LANES * (tile + 1)],
                    )
                    if tile < 2:
                        local = left_ref[first + 2 * unit + tile, picks, :]
                        local = jnp.concatenate([local, local], axis=1)
                    else:
                        one = right_ref[first + 2 * unit, picks, :]
                        two = right_ref[first + 2 * unit + 1, picks, :]
                        local = jnp.concatenate([one, two], axis=1)
                    heavy_ref[unit, parity, tile, :half] = (result[:half] * local).astype(bf16)
                    heavy_ref[unit, parity, tile, half:] = (result[half:] * local).astype(bf16)

    def backward_lines(unit):
        if True:
            for tile in range(3):
                even = dot(half_ref[2], heavy_ref[unit, 0, tile])
                odd = dot(half_ref[3], heavy_ref[unit, 1, tile])
                for side, values in enumerate((even + odd, even - odd)):
                    for low in range(half_owners):
                        owner = low + side * half_owners
                        for part in range(2):
                            start = part * half + low * slab
                            found = values[start : start + slab]
                            one, two = found[:, :LANES], found[:, LANES:]
                            if tile < 2:
                                rows = pl.ds(
                                    pl.multiple_of((2 * unit + tile) * 2 * slab, 2 * slab), 2 * slab
                                )
                                after_ref[owner, rows, part * LANES : (part + 1) * LANES] = (
                                    jnp.concatenate([one, two], axis=0).astype(bf16)
                                )
                            else:
                                for place, both in enumerate((one, two)):
                                    plane = 2 * unit + place
                                    rows = pl.ds(
                                        pl.multiple_of(plane * 2 * slab, 2 * slab), 2 * slab
                                    )
                                    after_ref[
                                        owner, rows, (2 + part) * LANES : (3 + part) * LANES
                                    ] = jnp.concatenate(
                                        [
                                            jnp.where(low_lane, both, 0.0),
                                            jnp.where(low_lane, 0.0, both),
                                        ],
                                        axis=0,
                                    ).astype(bf16)

    part_row = lax.broadcasted_iota(jnp.int32, (CHUNK, LANES), 0)
    part_row = jnp.bitwise_and(part_row, PLANES) == 0

    def weighed_lines():
        for owner in range(owners):
            result = dot(after_ref[owner], again_ref[owner])
            mask = mask_ref[owner] * scale
            mask = jnp.concatenate([mask, mask], axis=1)[None]
            kept = (result.reshape(lines, slab, 2 * LANES) * mask).reshape(lines * slab, 2 * LANES)
            kept_ref[owner] = kept.astype(bf16)

    def picked_lines(place):
        for owner in range(owners):
            found = dot(pick_ref[...], kept_ref[owner])
            stage_ref[place, owner] = jnp.where(
                part_row, found[:, :LANES], found[:, LANES:]
            ).astype(bf16)

    def wait_batch(batch):
        some = slice(bounds[batch], bounds[batch + 1])
        await_bytes(stick_ref.at[some, : owners - 1], recv_sem.at[batch])

    def send_home(group):
        for place in range(owners - 1):
            home_copy(group, place).start()
        back_ref[group, me] = stage_ref[group + 2, me]

    for place in range(owners - 1):
        there_copy(2, place).start()
    wait_batch(0)
    spread_lines(0)
    for unit in range(PLANES // 2):
        forward_lines(0, unit)
    for unit in range(PLANES // 2):
        backward_lines(unit)
    spread_lines(1)

    @pl.loop(1, groups - 1)
    def _(group):
        for batch in (1, 2):

            @pl.when(group + 1 == bounds[batch])
            def _():
                wait_batch(batch)

        for unit in range(PLANES // 2):
            forward_lines(group, unit)
        picked_lines(group)
        weighed_lines()
        for unit in range(PLANES // 2):
            backward_lines(unit)
        spread_lines(group + 1)

        @pl.when(group > 1)
        def _():
            send_home(group - 2)

    for unit in range(PLANES // 2):
        forward_lines(groups - 1, unit)
    picked_lines(groups - 1)
    weighed_lines()
    for unit in range(PLANES // 2):
        backward_lines(unit)
    picked_lines(groups)
    weighed_lines()
    picked_lines(groups + 1)
    for group in range(groups - 3, groups):
        send_home(group)

    def gather_waves(pair):
        first = pair * groups_pair

        @pl.loop(0, groups_pair)
        def _(step):
            await_bytes(back_ref.at[first + step, : owners - 1], home_recv.at[first + step])

        chunks = back_ref[first : first + groups_pair].reshape(groups_pair * owners, CHUNK, LANES)
        chunks = chunks.astype(f32)
        columns = []
        for band in range(PAIR):
            rows = chunks[:, band * 2 * PLANES : (band + 1) * 2 * PLANES]
            columns.append(rows.reshape(2 * size, LANES))
        columns = jnp.concatenate(columns, axis=1).astype(bf16)
        risen = (halves_dot(rise_ref, columns) * (1.0 / size)).astype(bf16)
        pieces = []
        for band in range(PAIR):
            for part in range(2):
                sides = []
                for side in range(FOLD):
                    start = part * size + side * fold
                    sides.append(risen[start : start + fold, band * LANES : (band + 1) * LANES])
                pieces.append(jnp.concatenate(sides, axis=1))
        gather_ref[...] = jnp.concatenate(pieces, axis=0)

        @pl.loop(0, blocks // 2, unroll=8)
        def _(step):
            values = dot(gather_ref[...], hot_ref[:, lanes_of(2 * step, 2)])
            for side in range(2):
                chosen = level_mask(2 * step + side)
                for part in range(2 * PAIR):
                    ours = values[part * fold : (part + 1) * fold, side * LANES : (side + 1) * LANES]
                    row = 2 * PAIR * pair + part
                    found_ref[row : row + 1, lanes_of(2 * step + side)] = jnp.sum(
                        jnp.where(chosen, ours, 0.0), axis=0, keepdims=True
                    )

    def find_kinetic():
        freq_x = jnp.where(grid_x >= half, grid_x - size, grid_x)
        freq_y = jnp.where(grid_y >= half, grid_y - size, grid_y)
        freq_row = lax.broadcasted_iota(jnp.int32, (16, LANES), 0)
        freqs = jnp.where(freq_row == 0, freq_x, jnp.where(freq_row == 1, freq_y, 0.0))
        freqs = jnp.concatenate([freqs] * FOLD, axis=1).astype(bf16)

        @pl.loop(0, blocks // 8)
        def _(step):
            found = dot(freqs, hot_ref[:, lanes_of(8 * step, 8)])
            plane = lax.shift_right_logical(slot_ref[:, lanes_of(8 * step, 8)], 7)
            freq_z = jnp.where(plane >= half, plane - size, plane).astype(f32)
            total = freq_z * freq_z + found[0:1] * found[0:1] + found[1:2] * found[1:2]
            kinetic_ref[:, lanes_of(8 * step, 8)] = total * (2.0 / (size * size))

    for pair in range(pairs):
        if pair == pairs - 1:
            find_kinetic()
        gather_waves(pair)

    result = found_ref[...] + kinetic_ref[...] * wave_ref[...]
    applied_ref[...] = result.astype(bf16).reshape(bands, 2, waves)

    inside = source_band == band_me

    @pl.when(inside)
    def _():
        await_bytes(shares_ref.at[: mesh_bands * shares - 1], once_sem.at[4])
        await_bytes(shares_ref.at[: owners - 1], once_sem.at[5])

    @pl.when(jnp.logical_not(inside))
    def _():
        await_bytes(shares_ref.at[: mesh_bands * shares], once_sem.at[4])
        await_bytes(shares_ref, once_sem.at[5])

    await_bytes(coords_ref.at[: owners - 1], once_sem.at[0])
    await_bytes(every_ref.at[: mesh_bands - 1], once_sem.at[2])
    await_bytes(stick_ref.at[:, : owners - 1], once_sem.at[6])
    await_bytes(back_ref.at[:, : owners - 1], once_sem.at[7])

    total = shares_ref[0]
    for source in range(1, owners):
        total = total + shares_ref[source]
    total = pltpu.roll(total, lax.rem(LANES - 2 * bands * band_me, LANES), 1).T
    for part in range(2):
        for band in range(bands):
            row = 2 * band + part
            inter_ref[part, band : band + 1, :] = total[row : row + 1]


def whole_work(mesh_bands, orbitals, slots, columns, potential, subspace, previous):
    slab, size, _ = potential.shape
    owners = size // slab
    groups_pair = slab // PLANES
    bands, _, waves = orbitals.shape
    groups = bands // PAIR * groups_pair
    half = size // 2
    lines = PLANES * PAIR
    mine = subspace.shape[0]
    share = mine * mesh_bands // owners
    deep, rise = column_tables(size, slab)
    line, turn = line_tables(size)
    halves = half_tables(size)
    pick = pick_table(slab)
    in_vmem = pl.BlockSpec(memory_space=pltpu.VMEM)
    anywhere = pl.BlockSpec(memory_space=pl.ANY)
    bf16, f32 = jnp.bfloat16, jnp.float32
    dma = pltpu.SemaphoreType.DMA
    return pl.pallas_call(
        functools.partial(whole_kernel, mesh_bands),
        out_shape=(
            pltpu.VMEM(orbitals.shape, bf16),
            pltpu.VMEM((2, bands, share), f32),
        ),
        in_specs=[anywhere] * 12,
        out_specs=(in_vmem, in_vmem),
        scratch_shapes=[
            pltpu.VMEM(orbitals.shape, bf16),
            pltpu.VMEM(slots.shape, jnp.int32),
            pltpu.VMEM(columns.shape, jnp.int32),
            pltpu.VMEM(previous.shape, bf16),
            pltpu.VMEM(pick.shape, bf16),
            pltpu.VMEM(subspace.shape, bf16),
            pltpu.VMEM(deep.shape, bf16),
            pltpu.VMEM(rise.shape, bf16),
            pltpu.VMEM(line.shape, bf16),
            pltpu.VMEM(turn.shape, bf16),
            pltpu.VMEM(halves.shape, bf16),
            pltpu.VMEM((slab, size, size), f32),
            pltpu.VMEM((slab, size, LANES), f32),
            pltpu.VMEM((slab, size, LANES), f32),
            pltpu.VMEM((2 * bands, waves), f32),
            pltpu.VMEM((2 * bands, waves), f32),
            pltpu.VMEM((1, waves), f32),
            pltpu.VMEM((FOLD * LANES, waves), bf16),
            pltpu.VMEM((2 * PAIR * size // FOLD, FOLD * LANES), bf16),
            pltpu.VMEM((groups, owners, CHUNK, LANES), bf16),
            pltpu.VMEM((groups, owners, CHUNK, LANES), bf16),
            pltpu.VMEM((8, LANES), f32),
            pltpu.VMEM((owners, 8, LANES), f32),
            pltpu.VMEM((owners, slab, LANES), f32),
            pltpu.VMEM((owners, 2 * LANES, 4 * LANES), bf16),
            pltpu.VMEM((owners, 4 * LANES, 2 * LANES), bf16),
            pltpu.VMEM((PLANES // 2, 2, size, 6 * LANES), bf16),
            pltpu.VMEM((PLANES // 2, 2, 3, size, 2 * LANES), bf16),
            pltpu.VMEM((owners, lines * slab, 4 * LANES), bf16),
            pltpu.VMEM((owners, lines * slab, 2 * LANES), bf16),
            pltpu.VMEM((groups + 2, owners, CHUNK, LANES), bf16),
            pltpu.VMEM((groups, owners, CHUNK, LANES), bf16),
            pltpu.VMEM((mesh_bands, bands, 2, waves), bf16),
            pltpu.VMEM((LANES, waves), bf16),
            pltpu.VMEM((2 * mine, LANES), f32),
            pltpu.VMEM((mine // share, share, LANES), f32),
            pltpu.VMEM((owners, share, LANES), f32),
            dma((13,)),
            dma((3,)),
            dma((groups,)),
            dma((8,)),
        ],
        compiler_params=pltpu.CompilerParams(
            collective_id=0, has_side_effects=True, vmem_limit_bytes=60 * 1024 * 1024
        ),
        cost_estimate=pl.CostEstimate(
            flops=40 * 10**9, bytes_accessed=8 * 10**6, transcendentals=0
        ),
    )(
        orbitals,
        slots,
        columns,
        previous,
        subspace,
        potential,
        deep,
        rise,
        line,
        turn,
        halves,
        pick,
    )


def fast_device(mesh_bands, orbitals, sphere_slot, stick_column, potential, subspace, previous):
    slots = sphere_slot.reshape(1, -1)
    columns = stick_column.reshape(1, -1)
    arrays = (orbitals, slots, columns, potential, subspace, previous)
    applied, turned = whole_work(mesh_bands, *arrays)
    return applied, turned.transpose(0, 2, 1)


def fits(mesh_bands, orbitals, slots, sticks, potential, subspace, previous):
    slab, size, _ = potential.shape
    owners = size // slab
    bands, mine = orbitals.shape[0], subspace.shape[0]
    good = slab % 8 == 0 and owners % 2 == 0 and owners * slab == size
    good = good and 2 * size == 3 * LANES and sticks.shape[0] == LANES
    good = good and bands % PAIR == 0 and slots.shape[0] % (8 * LANES) == 0
    good = good and mine * mesh_bands % (8 * owners) == 0 and owners % mesh_bands == 0
    return good and 2 * mesh_bands * bands <= LANES


def per_device(mesh_bands, *arrays):
    if fits(mesh_bands, *arrays):
        return fast_device(mesh_bands, *arrays)
    return general_device(*arrays)


def solution(mesh):
    return jax.shard_map(
        functools.partial(per_device, mesh.shape["band"]),
        mesh=mesh,
        in_specs=(
            P("band", None, "fft"),
            P("fft"),
            P("fft"),
            P("fft", None, None),
            P("band", None, "fft"),
            P("band", None, "fft"),
        ),
        out_specs=(P("band", None, "fft"), P(None, "fft", "band")),
        check_vma=False,
    )
```

```python
import functools
import math

import jax
import jax.numpy as jnp
import numpy as np
from jax import lax
from jax.experimental import pallas as pl
from jax.experimental.pallas import tpu as pltpu
from jax.sharding import PartitionSpec as P


def dft_table(length, sign_value, factor):
    positions = jnp.arange(length, dtype=jnp.int32)
    phase_step = positions[:, None] * positions[None, :] % length
    angle_value = phase_step.astype(jnp.float32) * (2.0 * math.pi / length)
    cosine = (jnp.cos(angle_value) * factor).astype(jnp.bfloat16)
    sine_part = (jnp.sin(angle_value) * (sign_value * factor)).astype(jnp.bfloat16)
    return (cosine, sine_part)


def apply_dft(real_in, imag_in, table, form):
    cosine, sine_part = table

    def product(operand, table_part):
        return jnp.einsum(form, operand, table_part, preferred_element_type=jnp.float32)

    real_out = product(real_in, cosine) - product(imag_in, sine_part)
    imag_out = product(real_in, sine_part) + product(imag_in, cosine)
    return (real_out, imag_out)


def packed(pair, axis_pos):
    return jnp.stack([pair[0].astype(jnp.bfloat16), pair[1].astype(jnp.bfloat16)], axis=axis_pos)


def frequency(values, grid_size):
    return jnp.where(values >= grid_size // 2, values - grid_size, values).astype(jnp.float32)


def one_hot_rows(indices, count):
    return (indices[None, :] == jnp.arange(count, dtype=jnp.int32)[:, None]).astype(jnp.bfloat16)


def general_device(orbitals, sphere_slot, stick_column, potential, subspace, previous):
    slab_depth = potential.shape[0]
    grid_size = potential.shape[1]
    stick_count = stick_column.shape[0]
    slab_cells = slab_depth * grid_size
    forward = dft_table(grid_size, 1.0, 1.0)
    inverse = dft_table(grid_size, -1.0, 1.0 / grid_size)
    plane_index = sphere_slot // stick_count
    stick_index = sphere_slot % stick_count
    plane_hot = one_hot_rows(plane_index, grid_size)
    stick_hot = one_hot_rows(stick_index, stick_count)
    stick_coords = jnp.stack([stick_column // grid_size, stick_column % grid_size]).astype(
        jnp.bfloat16
    )
    wave_coords = jnp.dot(stick_coords, stick_hot, preferred_element_type=jnp.float32)
    freq_z = frequency(plane_index, grid_size)
    freq_x = frequency(wave_coords[0].astype(jnp.int32), grid_size)
    freq_y = frequency(wave_coords[1].astype(jnp.int32), grid_size)
    kinetic = (freq_z * freq_z + freq_x * freq_x + freq_y * freq_y) * (
        2.0 / (grid_size * grid_size)
    )
    prev_real = previous[:, 0]
    prev_imag = previous[:, 1]
    sub_piece = lax.all_gather(subspace, "band", axis=0, tiled=True)
    sub_real = sub_piece[:, 0]
    sub_imag = sub_piece[:, 1]
    over_real = jnp.einsum(
        "jg,ig->ji", sub_real, prev_real, preferred_element_type=jnp.float32
    ) + jnp.einsum("jg,ig->ji", sub_imag, prev_imag, preferred_element_type=jnp.float32)
    over_imag = jnp.einsum(
        "jg,ig->ji", sub_real, prev_imag, preferred_element_type=jnp.float32
    ) - jnp.einsum("jg,ig->ji", sub_imag, prev_real, preferred_element_type=jnp.float32)
    partial_value = jnp.stack([over_real, over_imag])
    intersection = lax.psum_scatter(partial_value, "fft", scatter_dimension=1, tiled=True)
    stick_buffer = jnp.einsum(
        "bpi,zi,si->bpzs", orbitals, plane_hot, stick_hot, preferred_element_type=jnp.float32
    ).astype(jnp.bfloat16)

    def potential_work(along_y):
        along_x = apply_dft(along_y[0], along_y[1], forward, "zxy,xk->zky")
        weighted = packed((along_x[0] * potential, along_x[1] * potential), 0)
        back_x = packed(apply_dft(weighted[0], weighted[1], inverse, "zxy,xk->zky"), 0)
        return packed(apply_dft(back_x[0], back_x[1], inverse, "zxy,yk->zxk"), 0)

    along_z = packed(apply_dft(stick_buffer[:, 0], stick_buffer[:, 1], forward, "bzs,zk->bks"), 1)
    all_columns = lax.all_gather(stick_column, "fft", axis=0, tiled=True)
    owners = all_columns.shape[0] // stick_count
    block_columns = (all_columns % slab_cells).reshape(owners, stick_count)
    block_hot = (
        block_columns[:, :, None] == jnp.arange(slab_cells, dtype=jnp.int32)[None, None, :]
    ).astype(jnp.bfloat16)

    def stick_work(one_band):
        plane_depth = one_band.shape[1]
        split_band = one_band.reshape(2, plane_depth, owners, stick_count)
        plane_grid = jnp.einsum(
            "pzds,dsc->pzdc", split_band, block_hot, preferred_element_type=jnp.float32
        ).astype(jnp.bfloat16)
        plane_grid = plane_grid.reshape(2, plane_depth, grid_size, grid_size)
        along_y = packed(apply_dft(plane_grid[0], plane_grid[1], forward, "zxy,yk->zxk"), 0)
        back_y = potential_work(along_y)
        back_split = back_y.reshape(2, plane_depth, owners, slab_cells)
        picked = jnp.einsum(
            "pzdc,dsc->pzds", back_split, block_hot, preferred_element_type=jnp.float32
        ).astype(jnp.bfloat16)
        return picked.reshape(2, plane_depth, owners * stick_count)

    finished = lax.map(
        stick_work, lax.all_to_all(along_z, "fft", split_axis=2, concat_axis=3, tiled=True)
    )
    stick_values = lax.all_to_all(finished, "fft", split_axis=3, concat_axis=2, tiled=True)
    picked_sticks = jnp.einsum(
        "bpzs,si->bpzi", stick_values, stick_hot, preferred_element_type=jnp.float32
    ).astype(jnp.bfloat16)
    cosine_cols = jnp.einsum("zk,ki->zi", inverse[0], plane_hot, preferred_element_type=jnp.float32)
    sine_cols = jnp.einsum("zk,ki->zi", inverse[1], plane_hot, preferred_element_type=jnp.float32)
    pick_real = picked_sticks[:, 0].astype(jnp.float32)
    pick_imag = picked_sticks[:, 1].astype(jnp.float32)
    wave_real = jnp.sum(pick_real * cosine_cols[None] - pick_imag * sine_cols[None], axis=1)
    wave_imag = jnp.sum(pick_real * sine_cols[None] + pick_imag * cosine_cols[None], axis=1)
    real_out = wave_real + kinetic * orbitals[:, 0].astype(jnp.float32)
    imag_out = wave_imag + kinetic * orbitals[:, 1].astype(jnp.float32)
    applied = jnp.stack([real_out, imag_out], axis=1).astype(jnp.bfloat16)
    return (applied, intersection)


PLANES = 4
PAIR = 2
LANES = 128
CHUNK = 4 * PLANES
FOLD = 4


def phases(products, length):
    angle = (products % length).astype(np.float64) * (2.0 * np.pi / length)
    return np.cos(angle), np.sin(angle)


def as_bf16(array):
    return jnp.asarray(array, jnp.bfloat16)


def line_tables(length):
    cosine, sine = phases(np.outer(np.arange(length), np.arange(length)), length)

    def spread(table):
        rest = table[:, LANES:]
        return table[:, :LANES], np.concatenate([rest, rest], axis=1)

    tables = []
    for to_real, to_imag in ((cosine, sine), (-sine, cosine)):
        real_main, real_rest = spread(to_real)
        imag_main, imag_rest = spread(to_imag)
        tables.append(np.concatenate([real_main, imag_main, real_rest, imag_rest], axis=1))
    there = np.stack(tables)
    return as_bf16(there), as_bf16(there.transpose(0, 2, 1))


def half_tables(length):
    half = np.arange(length // 2)
    natural = np.arange(length).reshape(2, length // 16, 8)
    mixed = natural.transpose(1, 0, 2).reshape(-1)
    there, back = [], []
    for parity in (0, 1):
        cosine, sine = phases(np.outer(2 * half + parity, half), length)
        table = np.block([[cosine, -sine], [sine, cosine]])
        there.append(table[:, mixed])
        back.append(table.T)
    return as_bf16(np.stack(there + back))


def column_tables(length, slab):
    cosine, sine = phases(np.outer(np.arange(length), np.arange(length)), length)
    table = np.block([[cosine, -sine], [sine, cosine]])
    order = np.arange(2 * length).reshape(2, length // slab, slab // PLANES, PLANES)
    order = order.transpose(2, 1, 0, 3).reshape(-1)
    there = table[order]
    return as_bf16(there), as_bf16(there.T)


def pick_table(slab):
    lines = PLANES * PAIR
    table = np.zeros((CHUNK, lines * slab))
    for plane in range(PLANES):
        for band in range(PAIR):
            line = plane * PAIR + band
            for part in range(2):
                row = band * 2 * PLANES + part * PLANES + plane
                table[row, line * slab : (line + 1) * slab] = 1.0
    return as_bf16(table)


def whole_kernel(
    mesh_bands,
    orbital_hbm,
    slot_hbm,
    column_hbm,
    previous_hbm,
    subspace_hbm,
    pot_ref,
    deep_hbm,
    rise_hbm,
    line_hbm,
    turn_hbm,
    half_hbm,
    pick_hbm,
    applied_ref,
    inter_ref,
    orbital_ref,
    slot_ref,
    column_ref,
    previous_ref,
    pick_ref,
    subspace_ref,
    deep_ref,
    rise_ref,
    line_ref,
    turn_ref,
    half_ref,
    full_ref,
    left_ref,
    right_ref,
    wave_ref,
    found_ref,
    kinetic_ref,
    hot_ref,
    gather_ref,
    sent_ref,
    stick_ref,
    coord_ref,
    coords_ref,
    mask_ref,
    there_ref,
    again_ref,
    mixed_ref,
    heavy_ref,
    after_ref,
    kept_ref,
    stage_ref,
    back_ref,
    every_ref,
    right_side_ref,
    blend_ref,
    share_ref,
    shares_ref,
    load_sem,
    recv_sem,
    home_recv,
    once_sem,
):
    slab, size, _ = pot_ref.shape
    owners = size // slab
    half_owners = owners // 2
    half = size // 2
    fold = size // FOLD
    groups_pair = slab // PLANES
    waves = slot_ref.shape[1]
    blocks = waves // LANES
    sticks = LANES
    lines = PLANES * PAIR
    bands = orbital_ref.shape[0]
    pairs = bands // PAIR
    groups = pairs * groups_pair
    rest = size - LANES
    scale = 1.0 / (size * size)
    mine = subspace_ref.shape[0]
    share = share_ref.shape[1]
    shares = mine // share
    me = lax.axis_index("fft")
    band_me = lax.axis_index("band")
    every_band = [lax.rem(band_me + shift, mesh_bands) for shift in range(mesh_bands)]
    others = [lax.rem(me + shift, owners) for shift in range(1, owners)]
    f32, bf16 = jnp.float32, jnp.bfloat16

    def dot(left, right):
        return jnp.dot(left, right, preferred_element_type=f32)

    def halves_dot(table_ref, right):
        return jnp.concatenate([dot(table_ref[:size], right), dot(table_ref[size:], right)], axis=0)

    def remote(src, dst, send, recv, target):
        return pltpu.make_async_remote_copy(
            src_ref=src,
            dst_ref=dst,
            send_sem=send,
            recv_sem=recv,
            device_id=target,
            device_id_type=pl.DeviceIdType.MESH,
        )

    def coord_copy(place):
        return remote(
            coord_ref,
            coords_ref.at[me],
            once_sem.at[0],
            once_sem.at[1],
            {"fft": others[place]},
        )

    def band_copy(place):
        return remote(
            previous_ref,
            every_ref.at[band_me],
            once_sem.at[2],
            once_sem.at[3],
            {"band": every_band[place + 1]},
        )

    def share_copy(block, place):
        return remote(
            share_ref.at[block],
            shares_ref.at[me],
            once_sem.at[4],
            once_sem.at[5],
            {"band": every_band[place], "fft": shares * band_me + block},
        )

    def await_bytes(region, sem):
        pltpu.make_async_copy(region, region, sem).wait()

    bounds = (0, 2, groups_pair, groups)

    def there_copy(batch, place):
        some = slice(bounds[batch], bounds[batch + 1])
        return remote(
            sent_ref.at[some, others[place]],
            stick_ref.at[some, me],
            once_sem.at[6],
            recv_sem.at[batch],
            {"fft": others[place]},
        )

    def home_copy(group, place):
        return remote(
            stage_ref.at[group + 2, others[place]],
            back_ref.at[group, me],
            once_sem.at[7],
            home_recv.at[group],
            {"fft": others[place]},
        )

    barrier = pltpu.get_barrier_semaphore()
    for place in range(mesh_bands):
        for other in [me] + others:
            if place or other is not me:
                pl.semaphore_signal(
                    barrier,
                    inc=1,
                    device_id={"band": every_band[place], "fft": other},
                    device_id_type=pl.DeviceIdType.MESH,
                )

    sides = (
        (slot_hbm, slot_ref),
        (orbital_hbm, orbital_ref),
        (column_hbm, column_ref),
        (previous_hbm, previous_ref),
        (deep_hbm, deep_ref),
        (line_hbm, line_ref),
        (turn_hbm, turn_ref),
        (subspace_hbm, subspace_ref),
        (pot_ref, full_ref),
        (half_hbm, half_ref),
        (pick_hbm, pick_ref),
        (rise_hbm, rise_ref),
    )
    loads = []
    for place, (src, dst) in enumerate(sides):
        loads.append(pltpu.make_async_copy(src, dst, load_sem.at[place]))
    for place in range(5):
        loads[place].start()
    for place in range(4):
        loads[place].wait()

    low_lane = lax.broadcasted_iota(jnp.int32, (1, LANES), 1) < rest
    level = lax.broadcasted_iota(jnp.int32, (fold, LANES), 0)
    wave_ref[...] = orbital_ref[...].reshape(2 * bands, waves).astype(f32)

    column = column_ref[...]
    grid_x = jnp.floor((column.astype(f32) + 0.5) * (1.0 / size))
    grid_y = column.astype(f32) - grid_x * size
    coord_row = lax.broadcasted_iota(jnp.int32, (8, LANES), 0)
    first_x = lax.convert_element_type(me * slab, f32)
    coord_ref[...] = jnp.where(coord_row == 0, grid_x - first_x, jnp.where(coord_row == 1, grid_y, 0.0))

    def lanes_of(block, count=1):
        return pl.ds(pl.multiple_of(block * LANES, LANES), count * LANES)

    def plane_of(block):
        return lax.shift_right_logical(slot_ref[:, lanes_of(block)], 7)

    def hot_of(block):
        stick = jnp.bitwise_and(slot_ref[:, lanes_of(block)], sticks - 1)
        plane = plane_of(block)
        rows = lax.broadcasted_iota(jnp.int32, (sticks, LANES), 0)
        chosen = jnp.where(stick == rows, 1.0, 0.0).astype(bf16).reshape(-1, 16, LANES)
        sides = []
        for side in range(FOLD):
            inside = jnp.logical_and(plane >= side * fold, plane < (side + 1) * fold)
            inside = jnp.broadcast_to(jnp.where(inside, 1.0, 0.0), (16, LANES)).astype(bf16)
            sides.append((chosen * inside[None]).reshape(sticks, LANES))
        return jnp.concatenate(sides, axis=0)

    for place in range(5, len(loads)):
        loads[place].start()
    coords_ref[me] = coord_ref[...]
    every_ref[band_me] = previous_ref[...]

    def level_mask(block):
        plane = plane_of(block)
        for side in range(1, FOLD):
            base = jnp.where(plane >= side * fold, side * fold, 0 if side == 1 else base)
        return plane - base == level

    cells = None
    for block in range(0, blocks, 2):
        pieces = []
        hot = jnp.concatenate([hot_of(block), hot_of(block + 1)], axis=1)
        hot_ref[:, lanes_of(block, 2)] = hot
        for step in range(2):
            chosen = level_mask(block + step)
            values = wave_ref[:, lanes_of(block + step)]
            rows = [jnp.where(chosen, values[row : row + 1], 0.0) for row in range(2 * bands)]
            pieces.append(jnp.concatenate(rows, axis=0))
        left = jnp.concatenate(pieces, axis=1).astype(bf16)
        term = lax.dot_general(
            left,
            hot,
            (((1,), (1,)), ((), ())),
            preferred_element_type=f32,
        )
        cells = term if cells is None else cells + term
    columns = []
    for band in range(bands):
        pieces = []
        for part in range(2):
            start = (2 * band + part) * fold
            for side in range(FOLD):
                pieces.append(cells[start : start + fold, side * LANES : (side + 1) * LANES])
        columns.append(jnp.concatenate(pieces, axis=0))
    columns = jnp.concatenate(columns, axis=1).astype(bf16)
    loads[4].wait()
    along = dot(deep_ref[...], columns).reshape(groups_pair * owners, 2 * PLANES, bands * LANES)
    for pair in range(pairs):
        chunks = []
        for band in range(PAIR * pair, PAIR * (pair + 1)):
            chunks.append(along[:, :, band * LANES : (band + 1) * LANES])
        sent_ref[pair * groups_pair : (pair + 1) * groups_pair] = (
            jnp.concatenate(chunks, axis=1)
            .astype(bf16)
            .reshape(groups_pair, owners, CHUNK, LANES)
        )

    pl.semaphore_wait(barrier, mesh_bands * owners - 1)
    for place in range(owners - 1):
        coord_copy(place).start()
    for batch in range(2):
        for place in range(owners - 1):
            there_copy(batch, place).start()
    for place in range(mesh_bands - 1):
        band_copy(place).start()
    stick_ref[:, me] = sent_ref[:, me]

    for place in range(5, len(loads)):
        loads[place].wait()

    @pl.loop(0, slab, unroll=4)
    def _(plane):
        local = full_ref[plane, :, LANES:]
        right_ref[plane] = jnp.concatenate([local, local], axis=1)
        left_ref[plane] = full_ref[plane, :, :LANES]

    await_bytes(coords_ref.at[: owners - 1], once_sem.at[1])

    @pl.loop(0, owners // 2, unroll=2)
    def _(step):
        local = lax.broadcasted_iota(jnp.int32, (slab, sticks), 0).astype(f32)
        cells = lax.broadcasted_iota(jnp.int32, (size, sticks), 0).astype(f32)
        hots = []
        for side in range(2):
            coords = coords_ref[2 * step + side]
            mask_ref[2 * step + side] = jnp.where(coords[0:1, :] == local, 1.0, 0.0)
            hots.append(jnp.where(coords[1:2, :] == cells, 1.0, 0.0))
        hot = jnp.concatenate(hots, axis=1).astype(bf16)
        for part in range(2):
            place = slice(part * sticks, (part + 1) * sticks)
            rows = lax.dot_general(
                hot, line_ref[part], (((0,), (0,)), ((), ())), preferred_element_type=f32
            ).astype(bf16)
            turned = dot(turn_ref[part], hot).astype(bf16)
            for side in range(2):
                mine_here = slice(side * sticks, (side + 1) * sticks)
                there_ref[2 * step + side, place, :] = rows[mine_here]
                again_ref[2 * step + side, :, place] = turned[:, mine_here]

    await_bytes(every_ref.at[: mesh_bands - 1], once_sem.at[3])

    count = mesh_bands * bands
    right_side_ref[: 2 * count] = every_ref[...].reshape(2 * count, waves)
    products = lax.dot_general(
        subspace_ref[...].reshape(2 * mine, waves),
        right_side_ref[...],
        (((1,), (1,)), ((), ())),
        preferred_element_type=f32,
    )
    below = pltpu.roll(products, 2 * mine - 1, 0)
    even_lane = jnp.bitwise_and(lax.broadcasted_iota(jnp.int32, (1, LANES), 1), 1) == 0
    blend_ref[...] = jnp.where(
        even_lane,
        products + pltpu.roll(below, LANES - 1, 1),
        products - pltpu.roll(below, 1, 1),
    )
    for block in range(shares):
        share_ref[block] = blend_ref[pl.ds(2 * share * block, share, 2), :]

    source_band = lax.div(me, shares)
    for block in range(shares):
        for place in range(mesh_bands):
            if place:
                share_copy(block, place).start()
            else:
                to_self = shares * band_me + block == me

                @pl.when(jnp.logical_not(to_self))
                def _():
                    share_copy(block, place).start()

                @pl.when(to_self)
                def _():
                    shares_ref[me] = share_ref[block]

    def spread_lines(group):
        for owner in range(owners):
            low, far = owner % half_owners, owner // half_owners
            values = stick_ref[group, owner].astype(f32)
            mask = mask_ref[owner]
            parts = []
            for part in range(2):
                pieces = []
                for plane in range(PLANES):
                    for band in range(PAIR):
                        row = band * 2 * PLANES + part * PLANES + plane
                        pieces.append(values[row : row + 1, :] * mask)
                parts.append(jnp.concatenate(pieces, axis=0))
            left = jnp.concatenate(parts, axis=1).astype(bf16)
            for tile in range(2):
                place = slice(2 * LANES * tile, 2 * LANES * (tile + 1))
                result = dot(left, there_ref[owner, :, place])
                for plane in range(PLANES):
                    unit, side = plane // 2, plane % 2
                    start = plane * PAIR * slab
                    for band in range(1 if tile else PAIR):
                        found = []
                        for part in range(2):
                            here = slice(part * LANES, (part + 1) * LANES)
                            one = result[start : start + slab, here]
                            two = result[start + slab : start + 2 * slab, here]
                            if tile:
                                mine_here = jnp.where(low_lane, one, two)
                            else:
                                mine_here = two if band else one
                            found.append(mine_here.reshape(-1, 8, LANES))
                        offset = 4 + side if tile else 2 * side + band
                        mixed_ref[
                            unit, far, offset, 2 * slab * low : 2 * slab * (low + 1)
                        ] = jnp.concatenate(found, axis=1).reshape(2 * slab, LANES).astype(bf16)

    def forward_lines(group, unit):
        first = lax.rem(group, groups_pair) * PLANES
        for tile in range(3):
            near, far = [
                jnp.concatenate(
                    [mixed_ref[unit, side, 2 * tile], mixed_ref[unit, side, 2 * tile + 1]], axis=1
                )
                for side in range(2)
            ]
            for parity in range(2):
                picks = pl.ds(parity, half, 2)
                result = dot(half_ref[parity], near - far if parity else near + far)
                if tile < 2:
                    one = left_ref[first + 2 * unit + tile, picks, :]
                    two = one
                else:
                    one = right_ref[first + 2 * unit, picks, :]
                    two = right_ref[first + 2 * unit + 1, picks, :]
                for side, local in enumerate((one, two)):
                    here = slice(side * LANES, (side + 1) * LANES)
                    for part in range(2):
                        rows = slice(part * half, (part + 1) * half)
                        heavy_ref[unit, parity, tile, side, rows] = (
                            result[rows, here] * local
                        ).astype(bf16)

    def backward_lines(unit):
        for tile in range(3):
            for parity in range(2):
                heavy = jnp.concatenate(
                    [heavy_ref[unit, parity, tile, 0], heavy_ref[unit, parity, tile, 1]], axis=1
                )
                values = dot(half_ref[2 + parity], heavy)
                for part in range(2):
                    for low in range(half_owners):
                        start = part * half + low * slab
                        found = values[start : start + slab]
                        one, two = found[:, :LANES], found[:, LANES:]
                        if tile < 2:
                            plane = 2 * unit + tile
                            after_ref[
                                parity, low, part, plane * 2 * slab : (plane + 1) * 2 * slab
                            ] = jnp.concatenate([one, two], axis=0).astype(bf16)
                            continue
                        for place, both in enumerate((one, two)):
                            plane = 2 * unit + place
                            after_ref[
                                parity, low, 2 + part, plane * 2 * slab : (plane + 1) * 2 * slab
                            ] = jnp.concatenate(
                                [jnp.where(low_lane, both, 0.0), jnp.where(low_lane, 0.0, both)],
                                axis=0,
                            ).astype(bf16)

    part_row = lax.broadcasted_iota(jnp.int32, (CHUNK, LANES), 0)
    part_row = jnp.bitwise_and(part_row, PLANES) == 0

    def weighed_lines():
        for low in range(half_owners):
            even, odd = [
                jnp.concatenate([after_ref[parity, low, lane] for lane in range(4)], axis=1)
                for parity in range(2)
            ]
            for side in range(2):
                owner = low + side * half_owners
                result = dot(even - odd if side else even + odd, again_ref[owner])
                mask = mask_ref[owner] * scale
                for part in range(2):
                    kept = result[:, part * LANES : (part + 1) * LANES].reshape(lines, slab, LANES)
                    kept_ref[owner, part] = (
                        (kept * mask[None]).reshape(lines * slab, LANES).astype(bf16)
                    )

    def picked_lines(place):
        for owner in range(owners):
            kept = jnp.concatenate([kept_ref[owner, 0], kept_ref[owner, 1]], axis=1)
            found = dot(pick_ref[...], kept)
            stage_ref[place, owner] = jnp.where(
                part_row, found[:, :LANES], found[:, LANES:]
            ).astype(bf16)

    def wait_batch(batch):
        some = slice(bounds[batch], bounds[batch + 1])
        await_bytes(stick_ref.at[some, : owners - 1], recv_sem.at[batch])

    def send_home(group):
        for place in range(owners - 1):
            home_copy(group, place).start()
        back_ref[group, me] = stage_ref[group + 2, me]

    for place in range(owners - 1):
        there_copy(2, place).start()
    wait_batch(0)
    spread_lines(0)
    for unit in range(PLANES // 2):
        forward_lines(0, unit)
    for unit in range(PLANES // 2):
        backward_lines(unit)
    spread_lines(1)

    @pl.loop(1, groups - 1)
    def _(group):
        for batch in (1, 2):

            @pl.when(group + 1 == bounds[batch])
            def _():
                wait_batch(batch)

        for unit in range(PLANES // 2):
            forward_lines(group, unit)
        picked_lines(group)
        weighed_lines()
        for unit in range(PLANES // 2):
            backward_lines(unit)
        spread_lines(group + 1)

        @pl.when(group > 1)
        def _():
            send_home(group - 2)

    for unit in range(PLANES // 2):
        forward_lines(groups - 1, unit)
    picked_lines(groups - 1)
    weighed_lines()
    for unit in range(PLANES // 2):
        backward_lines(unit)
    picked_lines(groups)
    weighed_lines()
    picked_lines(groups + 1)
    for group in range(groups - 3, groups):
        send_home(group)

    def gather_waves(pair):
        first = pair * groups_pair

        @pl.loop(0, groups_pair)
        def _(step):
            await_bytes(back_ref.at[first + step, : owners - 1], home_recv.at[first + step])

        chunks = back_ref[first : first + groups_pair].reshape(groups_pair * owners, CHUNK, LANES)
        chunks = chunks.astype(f32)
        columns = []
        for band in range(PAIR):
            rows = chunks[:, band * 2 * PLANES : (band + 1) * 2 * PLANES]
            columns.append(rows.reshape(2 * size, LANES))
        columns = jnp.concatenate(columns, axis=1).astype(bf16)
        risen = (halves_dot(rise_ref, columns) * (1.0 / size)).astype(bf16)
        pieces = []
        for band in range(PAIR):
            for part in range(2):
                sides = []
                for side in range(FOLD):
                    start = part * size + side * fold
                    sides.append(risen[start : start + fold, band * LANES : (band + 1) * LANES])
                pieces.append(jnp.concatenate(sides, axis=1))
        gather_ref[...] = jnp.concatenate(pieces, axis=0)

        @pl.loop(0, blocks // 2, unroll=8)
        def _(step):
            values = dot(gather_ref[...], hot_ref[:, lanes_of(2 * step, 2)])
            for side in range(2):
                chosen = level_mask(2 * step + side)
                for part in range(2 * PAIR):
                    ours = values[part * fold : (part + 1) * fold, side * LANES : (side + 1) * LANES]
                    row = 2 * PAIR * pair + part
                    found_ref[row : row + 1, lanes_of(2 * step + side)] = jnp.sum(
                        jnp.where(chosen, ours, 0.0), axis=0, keepdims=True
                    )

    def find_kinetic():
        freq_x = jnp.where(grid_x >= half, grid_x - size, grid_x)
        freq_y = jnp.where(grid_y >= half, grid_y - size, grid_y)
        freq_row = lax.broadcasted_iota(jnp.int32, (16, LANES), 0)
        freqs = jnp.where(freq_row == 0, freq_x, jnp.where(freq_row == 1, freq_y, 0.0))
        freqs = jnp.concatenate([freqs] * FOLD, axis=1).astype(bf16)

        @pl.loop(0, blocks // 8)
        def _(step):
            found = dot(freqs, hot_ref[:, lanes_of(8 * step, 8)])
            plane = lax.shift_right_logical(slot_ref[:, lanes_of(8 * step, 8)], 7)
            freq_z = jnp.where(plane >= half, plane - size, plane).astype(f32)
            total = freq_z * freq_z + found[0:1] * found[0:1] + found[1:2] * found[1:2]
            kinetic_ref[:, lanes_of(8 * step, 8)] = total * (2.0 / (size * size))

    for pair in range(pairs):
        if pair == pairs - 1:
            find_kinetic()
        gather_waves(pair)

    result = found_ref[...] + kinetic_ref[...] * wave_ref[...]
    applied_ref[...] = result.astype(bf16).reshape(bands, 2, waves)

    inside = source_band == band_me

    @pl.when(inside)
    def _():
        await_bytes(shares_ref.at[: mesh_bands * shares - 1], once_sem.at[4])
        await_bytes(shares_ref.at[: owners - 1], once_sem.at[5])

    @pl.when(jnp.logical_not(inside))
    def _():
        await_bytes(shares_ref.at[: mesh_bands * shares], once_sem.at[4])
        await_bytes(shares_ref, once_sem.at[5])

    await_bytes(coords_ref.at[: owners - 1], once_sem.at[0])
    await_bytes(every_ref.at[: mesh_bands - 1], once_sem.at[2])
    await_bytes(stick_ref.at[:, : owners - 1], once_sem.at[6])
    await_bytes(back_ref.at[:, : owners - 1], once_sem.at[7])

    total = shares_ref[0]
    for source in range(1, owners):
        total = total + shares_ref[source]
    total = pltpu.roll(total, lax.rem(LANES - 2 * bands * band_me, LANES), 1).T
    for part in range(2):
        for band in range(bands):
            row = 2 * band + part
            inter_ref[part, band : band + 1, :] = total[row : row + 1]


def whole_work(mesh_bands, orbitals, slots, columns, potential, subspace, previous):
    slab, size, _ = potential.shape
    owners = size // slab
    groups_pair = slab // PLANES
    bands, _, waves = orbitals.shape
    groups = bands // PAIR * groups_pair
    half = size // 2
    lines = PLANES * PAIR
    mine = subspace.shape[0]
    share = mine * mesh_bands // owners
    deep, rise = column_tables(size, slab)
    line, turn = line_tables(size)
    halves = half_tables(size)
    pick = pick_table(slab)
    in_vmem = pl.BlockSpec(memory_space=pltpu.VMEM)
    anywhere = pl.BlockSpec(memory_space=pl.ANY)
    bf16, f32 = jnp.bfloat16, jnp.float32
    dma = pltpu.SemaphoreType.DMA
    return pl.pallas_call(
        functools.partial(whole_kernel, mesh_bands),
        out_shape=(
            pltpu.VMEM(orbitals.shape, bf16),
            pltpu.VMEM((2, bands, share), f32),
        ),
        in_specs=[anywhere] * 12,
        out_specs=(in_vmem, in_vmem),
        scratch_shapes=[
            pltpu.VMEM(orbitals.shape, bf16),
            pltpu.VMEM(slots.shape, jnp.int32),
            pltpu.VMEM(columns.shape, jnp.int32),
            pltpu.VMEM(previous.shape, bf16),
            pltpu.VMEM(pick.shape, bf16),
            pltpu.VMEM(subspace.shape, bf16),
            pltpu.VMEM(deep.shape, bf16),
            pltpu.VMEM(rise.shape, bf16),
            pltpu.VMEM(line.shape, bf16),
            pltpu.VMEM(turn.shape, bf16),
            pltpu.VMEM(halves.shape, bf16),
            pltpu.VMEM((slab, size, size), f32),
            pltpu.VMEM((slab, size, LANES), f32),
            pltpu.VMEM((slab, size, LANES), f32),
            pltpu.VMEM((2 * bands, waves), f32),
            pltpu.VMEM((2 * bands, waves), f32),
            pltpu.VMEM((1, waves), f32),
            pltpu.VMEM((FOLD * LANES, waves), bf16),
            pltpu.VMEM((2 * PAIR * size // FOLD, FOLD * LANES), bf16),
            pltpu.VMEM((groups, owners, CHUNK, LANES), bf16),
            pltpu.VMEM((groups, owners, CHUNK, LANES), bf16),
            pltpu.VMEM((8, LANES), f32),
            pltpu.VMEM((owners, 8, LANES), f32),
            pltpu.VMEM((owners, slab, LANES), f32),
            pltpu.VMEM((owners, 2 * LANES, 4 * LANES), bf16),
            pltpu.VMEM((owners, 4 * LANES, 2 * LANES), bf16),
            pltpu.VMEM((PLANES // 2, 2, 6, size, LANES), bf16),
            pltpu.VMEM((PLANES // 2, 2, 3, 2, size, LANES), bf16),
            pltpu.VMEM((2, owners // 2, 4, lines * slab, LANES), bf16),
            pltpu.VMEM((owners, 2, lines * slab, LANES), bf16),
            pltpu.VMEM((groups + 2, owners, CHUNK, LANES), bf16),
            pltpu.VMEM((groups, owners, CHUNK, LANES), bf16),
            pltpu.VMEM((mesh_bands, bands, 2, waves), bf16),
            pltpu.VMEM((LANES, waves), bf16),
            pltpu.VMEM((2 * mine, LANES), f32),
            pltpu.VMEM((mine // share, share, LANES), f32),
            pltpu.VMEM((owners, share, LANES), f32),
            dma((12,)),
            dma((3,)),
            dma((groups,)),
            dma((8,)),
        ],
        compiler_params=pltpu.CompilerParams(
            collective_id=0, has_side_effects=True, vmem_limit_bytes=60 * 1024 * 1024
        ),
        cost_estimate=pl.CostEstimate(
            flops=40 * 10**9, bytes_accessed=8 * 10**6, transcendentals=0
        ),
    )(
        orbitals,
        slots,
        columns,
        previous,
        subspace,
        potential,
        deep,
        rise,
        line,
        turn,
        halves,
        pick,
    )


def fast_device(mesh_bands, orbitals, sphere_slot, stick_column, potential, subspace, previous):
    slots = sphere_slot.reshape(1, -1)
    columns = stick_column.reshape(1, -1)
    arrays = (orbitals, slots, columns, potential, subspace, previous)
    applied, turned = whole_work(mesh_bands, *arrays)
    return applied, turned.transpose(0, 2, 1)


def fits(mesh_bands, orbitals, slots, sticks, potential, subspace, previous):
    slab, size, _ = potential.shape
    owners = size // slab
    bands, mine = orbitals.shape[0], subspace.shape[0]
    good = slab % 8 == 0 and owners % 2 == 0 and owners * slab == size
    good = good and 2 * size == 3 * LANES and sticks.shape[0] == LANES
    good = good and bands % PAIR == 0 and slots.shape[0] % (8 * LANES) == 0
    good = good and mine * mesh_bands % (8 * owners) == 0 and owners % mesh_bands == 0
    return good and 2 * mesh_bands * bands <= LANES


def per_device(mesh_bands, *arrays):
    if fits(mesh_bands, *arrays):
        return fast_device(mesh_bands, *arrays)
    return general_device(*arrays)


def solution(mesh):
    return jax.shard_map(
        functools.partial(per_device, mesh.shape["band"]),
        mesh=mesh,
        in_specs=(
            P("band", None, "fft"),
            P("fft"),
            P("fft"),
            P("fft", None, None),
            P("band", None, "fft"),
            P("band", None, "fft"),
        ),
        out_specs=(P("band", None, "fft"), P(None, "fft", "band")),
        check_vma=False,
    )
```
